256 devices in a mesh: row: 8 (over y, core), col: 32 (over z, x).
Axes of the slice: x: 4, y: 4, z: 8, core: 2. Of those that a mesh axis runs over, the one named last changes fastest.
Arguments:
- factor: float32 [6, 2048, 6, 2048], P(None, 'row', None, 'col'), may hold values from -0.0625 to 0.0625
- diag_inv: float32 [6, 2048, 2048], P(None, None, 'row'), may hold values from -2 to 2, as said below
- structure: int32 [6, 6, 16], P(None, None, 'row'), may hold values 0 or 1
- parent: int32 [6], replicated, may hold values from 1 to 6, as said below
- post: float32 [6, 2048, 64], P(None, 'row', 'col'), may hold values from -6 to 6
Outputs:
- mean_x: float32 [6, 2048, 64], P(None, 'row', 'col')
- variance: float32 [6, 2048], P(None, 'row')
The draws below stay inside these ranges and needn't reach their ends.
Inputs may be any that keep to these rules, and one draw needn't show every extreme that they name: parent[s] > s for s < 5, and parent[5] = 6; every supernode has at most 2 ancestors, and some supernode has exactly that many. The diagonal of each diag_inv[s] lies in 0.5 to 2.
All inputs are finite; a program needn't handle non-finite values. No bound on the sum of `structure` on one device may be relied on, other than what follows from the above.
Results may differ from the reference program's by a relative error of at most 0.00014.
Values sent between devices are 32-bit elements; how exact they have to be, the bound alone decides.
No kernel may reach another device: no remote copies, remote signals or barrier semaphores. Data moves between devices by JAX's collectives and lax.ppermute only.
A program may use at most 128 MiB of HBM per device.

```python
import math
import jax
import jax.numpy as jnp
from jax import lax

W = 2048
NSUP = 6
LEVELS = 3
RB = 128
NRHS = 64
NBLK = 16


def draw_diag_inv(key, part):
    key_lower = jax.random.fold_in(key, 11)
    key_diagonal = jax.random.fold_in(key, 12)
    lower_part = jax.random.truncated_normal(key_lower, -4.0, 4.0, (NSUP, W, W), jnp.float32) * (0.5 / math.sqrt(W))
    diagonal = jnp.exp(jax.random.uniform(key_diagonal, (NSUP, W), jnp.float32, math.log(0.5), math.log(2.0)))
    identity = jnp.eye(W, dtype=jnp.float32)
    return lower_part * (1.0 - identity) + diagonal[:, :, None] * identity


def draw_parent(key, part):
    slot_ids = jnp.arange(NSUP + 1, dtype=jnp.int32)
    parent = jnp.full((NSUP,), NSUP, jnp.int32)
    depths = jnp.zeros((NSUP + 1,), jnp.int32)
    for member in range(NSUP - 2, -1, -1):
        if member >= NSUP - LEVELS:
            chosen = jnp.int32(member + 1)
        else:
            eligible = ((slot_ids > member) & (slot_ids < NSUP) & (depths <= LEVELS - 2)).astype(jnp.int32)
            eligible_count = jnp.sum(eligible)
            drawn_slot = jax.random.randint(jax.random.fold_in(key, member), (), 0, eligible_count)
            running = jnp.cumsum(eligible)
            chosen = jnp.argmax((running == drawn_slot + 1) & (eligible == 1)).astype(jnp.int32)
        parent = parent.at[member].set(chosen)
        depths = depths.at[member].set(depths[chosen] + 1)
    return parent


def plant(array, stream_key, low, high):
    spot = [jax.random.randint(jax.random.fold_in(stream_key, axis), (), 0, length) for axis, length in enumerate(array.shape)]
    widest = array.shape.index(max(array.shape))
    neighbour = spot[:widest] + [(spot[widest] + 1) % array.shape[widest]] + spot[widest + 1:]
    return array.at[tuple(spot)].set(low).at[tuple(neighbour)].set(high)


def steps_of(stream_key, dims, shards, smallest, high):
    gain, own = 1.0, jax.random.fold_in(stream_key, 6)
    for position, shards_of in shards:
        draws = jnp.exp(jax.random.uniform(jax.random.fold_in(own, position), (shards_of,), jnp.float32, smallest / len(shards), high / len(shards)))
        gain = gain * jnp.repeat(draws, dims[position] // shards_of).reshape([-1 if axis == position else 1 for axis in range(len(dims))])
    return gain


def gaussian(rng, extent, spread, bound, shards=(), held_as=jnp.bfloat16):
    result = spread * jax.random.normal(rng, extent, jnp.float32)
    if shards:
        result = result * steps_of(rng, extent, shards, -0.22, 0.18)
    return jnp.clip(result, -bound, bound).astype(held_as)


def setup_inputs(seed: int = 0) -> dict:
    key_of = jax.random.split(jax.random.key(seed), 6)
    return {
        "factor": gaussian(key_of[0], (NSUP, W, NSUP, W), (4 * W) ** -0.5, 0.0625, ((1, 8), (3, 32)), jnp.float32),
        "diag_inv": draw_diag_inv(jax.random.fold_in(key_of[5], 71), 0),
        "structure": plant((jax.random.randint(key_of[2], (NSUP, NSUP, NBLK), 0, 4) < 3).astype(jnp.int32), jax.random.fold_in(key_of[2], 1), 0, 1),
        "parent": draw_parent(jax.random.fold_in(key_of[5], 71), 0),
        "post": gaussian(key_of[4], (NSUP, W, NRHS), 1.0, 6.0, ((1, 8), (2, 32)), jnp.float32),
    }


def ancestor_table(parent, super_count):
    extended = jnp.concatenate([parent, jnp.full((1,), super_count, jnp.int32)])
    slot_ids = jnp.arange(super_count + 1, dtype=jnp.int32)
    targets = jnp.arange(super_count, dtype=jnp.int32)
    current = parent
    table = jnp.zeros((super_count, super_count), jnp.float32)
    for hop_index in range(super_count - 1):
        table = table + (current[:, None] == targets[None, :]).astype(jnp.float32)
        onehot = (current[:, None] == slot_ids[None, :]).astype(jnp.int32)
        current = jnp.sum(onehot * extended[None, :], axis=1).astype(jnp.int32)
    return table


def reference(factor, diag_inv, structure, parent, post):
    ancestry = ancestor_table(parent, NSUP)
    row_mask = jnp.repeat(structure.astype(jnp.float32), RB, axis=2) * ancestry[:, :, None]
    lower_inv = jnp.tril(diag_inv)
    order_total = NSUP * W
    solved = [None] * NSUP
    for current_sup in range(NSUP - 1, -1, -1):
        unit_rows = jnp.eye(W, order_total, k=current_sup * W, dtype=jnp.float32)
        right = jnp.concatenate([post[current_sup], unit_rows], axis=1)
        for later in range(current_sup + 1, NSUP):
            block = factor[later, :, current_sup, :] * row_mask[current_sup, later][:, None]
            right = right - jnp.dot(block.T, solved[later], precision=lax.Precision.HIGHEST, preferred_element_type=jnp.float32)
        solved[current_sup] = jnp.dot(lower_inv[current_sup].T, right, precision=lax.Precision.HIGHEST, preferred_element_type=jnp.float32)
    solution = jnp.stack(solved)
    mean_x = solution[:, :, :NRHS]
    unit_part = solution[:, :, NRHS:]
    variance = jnp.sum(unit_part * unit_part, axis=2)
    return mean_x, variance
```

```python
import jax
import jax.numpy as jnp
from jax import lax
from jax.sharding import Mesh
from jax.sharding import PartitionSpec as P

ROW = ("y", "core")
COL = ("z", "x")
HIGH = lax.Precision.HIGH
HIGHEST = lax.Precision.HIGHEST


def shifted(array, axis, step):
    size = lax.axis_size(axis)
    return lax.ppermute(array, axis, [(i, (i + step) % size) for i in range(size)])


def pick(array, index, dim=0):
    return lax.dynamic_index_in_dim(array, index, dim, keepdims=False)


def gathered(array, axis):
    size = lax.axis_size(axis)
    at = lax.axis_index(axis)
    pieces = [array] + [shifted(array, axis, step) for step in range(1, size)]
    out = jnp.zeros((size, *array.shape), array.dtype)
    for step, piece in enumerate(pieces):
        out = lax.dynamic_update_index_in_dim(out, piece, (at - step) % size, 0)
    return out


def ring_gathered(array, axis):
    size = lax.axis_size(axis)
    at = lax.axis_index(axis)
    out = jnp.zeros((size, *array.shape), array.dtype)
    out = lax.dynamic_update_index_in_dim(out, array, at, 0)
    up = down = array
    for step in range(1, size // 2 + 1):
        if step < size // 2:
            up = shifted(up, axis, 1)
            down = shifted(down, axis, size - 1)
            out = lax.dynamic_update_index_in_dim(out, up, (at - step) % size, 0)
            out = lax.dynamic_update_index_in_dim(out, down, (at + step) % size, 0)
        else:
            half = array.shape[0] // 2
            first = shifted(up[:half], axis, 1)
            second = shifted(down[half:], axis, size - 1)
            piece = jnp.concatenate([first, second], axis=0)
            out = lax.dynamic_update_index_in_dim(out, piece, (at + step) % size, 0)
    return out


def row_scattered(parts):
    core = lax.axis_index("core")
    at = lax.axis_index("y")
    mine = pick(parts, core, 1)
    other = pick(parts, 1 - core, 1)
    paired = mine + shifted(other, "core", 1)
    total = pick(paired, at)
    for step in range(1, lax.axis_size("y")):
        total = total + shifted(pick(paired, (at + step) % lax.axis_size("y")), "y", step)
    return total


def row_gathered(array):
    near = gathered(array, "y")
    far = shifted(near, "core", 1)
    core = lax.axis_index("core")
    first = jnp.where(core == 0, near, far)
    second = jnp.where(core == 0, far, near)
    both = jnp.stack([first, second], axis=1)
    return both.reshape(-1, *array.shape)


def body(factor, diag_inv, structure, parent, post):
    count, height = factor.shape[0], factor.shape[1]
    narrow = factor.shape[3]
    full = diag_inv.shape[1]
    rhs = post.shape[2]
    y_at, core_at = lax.axis_index("y"), lax.axis_index("core")
    z_at, x_at = lax.axis_index("z"), lax.axis_index("x")
    zs, xs = lax.axis_size("z"), lax.axis_size("x")
    rows = lax.axis_size(ROW)
    ys = lax.axis_size("y")
    row_at = lax.axis_index(ROW)
    wide = narrow * xs
    strip = full // xs
    chunk = strip // zs
    fine = chunk // rows

    ids = jnp.arange(count, dtype=jnp.int32)
    has_parent = parent < count
    has_child = jnp.any(parent[:, None] == ids[None, :], axis=0)
    inner = has_parent & has_child
    outer = has_parent & ~has_child

    def slots(member, number):
        rank = jnp.sum((member[None, :] & (ids[None, :] < ids[:, None])).astype(jnp.int32), axis=1)
        hit = member[None, :] & (rank[None, :] == jnp.arange(number, dtype=jnp.int32)[:, None])
        return jnp.sum(hit * ids[None, :], axis=1).astype(jnp.int32), jnp.any(hit, axis=1)

    q_ids, q_ok = slots(inner, 2)
    o_ids, o_ok = slots(outer, 4)
    extended = jnp.concatenate([parent, jnp.full((1,), count, jnp.int32)])

    def parent_of(nodes):
        onehot = nodes[:, None] == jnp.arange(count + 1, dtype=jnp.int32)[None, :]
        return jnp.sum(onehot * extended[None, :], axis=1).astype(jnp.int32)

    q_par = parent_of(q_ids)
    o_par = parent_of(o_ids)
    o_grand = parent_of(o_par)
    o_has = o_ok & (o_par < count)
    o_deep = o_ok & (o_grand < count)
    o_slot = jnp.sum((o_par[:, None] == q_ids[None, :]) & q_ok[None, :] & (jnp.arange(2)[None, :] == 1), axis=1).astype(jnp.int32)
    q_par = jnp.minimum(q_par, count - 1)
    o_par = jnp.minimum(o_par, count - 1)
    o_grand = jnp.minimum(o_grand, count - 1)

    scale = structure.astype(jnp.float32)
    block_rows = height // structure.shape[2]

    def block(t, s, ok):
        piece = lax.dynamic_slice(factor, (t, 0, s, 0), (1, height, 1, narrow)).reshape(height, narrow)
        marks = lax.dynamic_slice(scale, (s, t, 0), (1, 1, structure.shape[2])).reshape(-1)
        marks = jnp.repeat(marks * ok.astype(jnp.float32), block_rows)
        return piece * marks[:, None]

    def widened(pairs):
        everyone = gathered(pairs, "x")
        cut = everyone.reshape(xs, *pairs.shape[:2], 2, narrow)
        cut = jnp.transpose(cut, (3, 1, 2, 0, 4))
        return cut.reshape(2, *pairs.shape[:2], wide)

    q_pack = jnp.concatenate([block(q_par[k], q_ids[k], q_ok[k]) for k in range(2)], axis=1)
    q_wide = widened(q_pack[None])[:, 0]
    o_pack = jnp.stack(
        [
            jnp.concatenate(
                [block(o_par[j], o_ids[j], o_has[j]), block(o_grand[j], o_ids[j], o_deep[j])], axis=1
            )
            for j in range(4)
        ]
    )
    o_wide = widened(o_pack)

    col_ids = row_at * height + jnp.arange(height, dtype=jnp.int32)
    lower = jnp.where((jnp.arange(full, dtype=jnp.int32)[:, None] >= col_ids[None, :])[None], diag_inv, 0.0)

    def strip_of(t):
        return lax.dynamic_slice(lower, (t, x_at * strip, 0), (1, strip, height))[0]

    def spread(partial):
        n = partial.shape[0]
        cut = partial.reshape(n, zs, ys, 2, fine, wide)
        cut = jnp.transpose(cut, (2, 3, 1, 0, 4, 5))
        own = row_scattered(cut)
        turned = lax.all_to_all(own, "z", 0, 0, tiled=True)
        everyone = row_gathered(turned)
        return jnp.transpose(everyone, (2, 0, 3, 1, 4)).reshape(n, chunk, full)

    def diag_of(t):
        return pick(lower, t)

    mul = lambda spec, a, b: jnp.einsum(spec, a, b, precision=HIGH, preferred_element_type=jnp.float32)

    q_strip = jnp.stack([strip_of(q_par[k]) for k in range(2)])
    q_rows = spread(-mul("nar,nrb->nab", q_strip, q_wide))
    q_done = mul("nak,nkw->naw", q_rows, jnp.stack([diag_of(q_ids[k]) for k in range(2)]))
    q_full = ring_gathered(q_done.reshape(2 * chunk, height), "z").reshape(zs, 2, chunk, height)
    q_full = jnp.transpose(q_full, (1, 0, 2, 3)).reshape(2, strip, height)

    o_diag = jnp.stack([diag_of(o_ids[j]) for j in range(4)])
    near_strip = jnp.stack([strip_of(o_par[j]) for j in range(4)])
    near_rows = spread(-mul("nar,nrb->nab", near_strip, o_wide[0]))
    near_done = mul("nak,nkw->naw", near_rows, o_diag)

    far_left = jnp.stack(
        [
            jnp.concatenate(
                [
                    pick(q_full, o_slot[j]) * o_deep[j].astype(jnp.float32),
                    strip_of(o_grand[j]),
                ],
                axis=1,
            )
            for j in range(4)
        ]
    )
    far_right = jnp.concatenate([o_wide[0], o_wide[1]], axis=1)
    far_rows = spread(-mul("nar,nrb->nab", far_left, far_right))
    far_done = mul("nak,nkw->naw", far_rows, o_diag)

    thin = jnp.transpose(post, (0, 2, 1)).reshape(count * rhs, height)
    tall = jnp.transpose(row_gathered(thin), (1, 0, 2)).reshape(count * rhs, xs, strip)
    by_x = lax.all_to_all(tall, "x", 1, 0, tiled=False)
    by_z = by_x.reshape(xs, count * rhs, zs, chunk)
    by_z = lax.all_to_all(by_z, "z", 2, 0, tiled=False)
    load = by_z.reshape(zs, xs, count, rhs, chunk)
    load = jnp.transpose(load, (2, 0, 1, 3, 4)).reshape(count, zs * xs * rhs, chunk)

    own = lax.dynamic_slice(lower, (0, x_at * strip + z_at * chunk, 0), (count, chunk, height))
    squares = jnp.sum(own * own, axis=1)
    means = mul("nbk,nkw->nbw", load, own)

    def onto(nodes):
        return (nodes[:, None] == ids[None, :]).astype(jnp.float32)

    q_load = jnp.stack([pick(load, q_par[k]) for k in range(2)])
    near_load = jnp.stack([pick(load, o_par[j]) for j in range(4)])
    far_load = jnp.stack([pick(load, o_grand[j]) for j in range(4)])
    q_mean = mul("nbk,nkw->nbw", q_load, q_done)
    o_mean = mul("nbk,nkw->nbw", near_load, near_done) + mul("nbk,nkw->nbw", far_load, far_done)
    q_square = jnp.sum(q_done * q_done, axis=1)
    o_square = jnp.sum(near_done * near_done, axis=1) + jnp.sum(far_done * far_done, axis=1)

    def placed(inner_part, outer_part, base):
        result = base
        for part, nodes in ((inner_part, q_ids), (outer_part, o_ids)):
            marks = onto(nodes)
            for k in range(part.shape[0]):
                result = result + marks[k].reshape(count, *([1] * (part.ndim - 1))) * part[k][None]
        return result

    squares = placed(q_square, o_square, squares)
    means = placed(q_mean, o_mean, means)

    cut = means.reshape(count, zs, xs, rhs, height)
    cut = jnp.transpose(cut, (2, 1, 3, 0, 4)).reshape(xs, zs * rhs, count, height)
    packed = jnp.concatenate([cut, jnp.broadcast_to(squares, (xs, 1, count, height))], axis=1)
    total = pick(packed, x_at)
    for step in range(1, xs):
        total = total + shifted(pick(packed, (x_at + step) % xs), "x", step)
    cut = total[: zs * rhs].reshape(zs, rhs, count, height)
    packed = jnp.concatenate([cut, jnp.broadcast_to(total[zs * rhs], (zs, 1, count, height))], axis=1)
    total = pick(packed, z_at)
    for step in range(1, zs):
        total = total + shifted(pick(packed, (z_at + step) % zs), "z", step)
    mean_x = jnp.transpose(total[:rhs], (1, 2, 0))
    return mean_x, total[rhs]


def solution(mesh):
    rows, cols = mesh.devices.shape
    finer = Mesh(mesh.devices.reshape(rows // 2, 2, cols // 4, 4), (*ROW, *COL))
    placed = (
        P(None, ROW, None, COL),
        P(None, None, ROW),
        P(None, None, ROW),
        P(),
        P(None, ROW, COL),
    )
    return jax.shard_map(
        body,
        mesh=finer,
        in_specs=placed,
        out_specs=(P(None, ROW, COL), P(None, ROW)),
        check_vma=False,
    )
```

```python
import functools

import jax
import jax.numpy as jnp
from jax import lax
from jax.experimental import pallas as pl
from jax.experimental.pallas import tpu as pltpu
from jax.sharding import Mesh
from jax.sharding import PartitionSpec as P

ROW = ("y", "core")
COL = ("z", "x")
F32 = jnp.float32
BF16 = jnp.bfloat16

N = 6
W = 2048
H = 256
YS, CS, ZS, XS = 4, 2, 8, 4
RS = YS * CS
NARROW = W // (ZS * XS)
WIDE = NARROW * XS
STRIP = W // XS
CHUNK = STRIP // ZS
FINE = CHUNK // RS
NQ, NO = 2, 4
RHS = 64

SMEM = pl.BlockSpec(memory_space=pltpu.SMEM)
VMEM = pl.BlockSpec(memory_space=pltpu.VMEM)
HBM = pl.BlockSpec(memory_space=pl.ANY)


def call(kernel, outs, in_specs, scratch):
    return pl.pallas_call(
        kernel,
        out_shape=outs,
        in_specs=in_specs,
        out_specs=jax.tree.map(lambda _: VMEM, outs),
        scratch_shapes=scratch,
        compiler_params=pltpu.CompilerParams(vmem_limit_bytes=56 * 1024 * 1024),
    )


def shape(*dims):
    return jax.ShapeDtypeStruct(dims, F32)


def tree_of(parent_ref):
    par = [parent_ref[i] for i in range(N)]
    zero = jnp.int32(0)
    q, q_ok, o, o_ok = [zero] * NQ, [zero] * NQ, [zero] * NO, [zero] * NO
    q_count = o_count = zero
    for i in range(N):
        has_parent = (par[i] < N).astype(jnp.int32)
        has_child = zero
        for s in range(i):
            has_child = has_child | (par[s] == i).astype(jnp.int32)
        inner = has_parent * has_child
        outer = has_parent * (1 - has_child)
        for k in range(NQ):
            hit = inner * (q_count == k).astype(jnp.int32)
            q[k] = jnp.where(hit == 1, i, q[k])
            q_ok[k] = q_ok[k] | hit
        for k in range(NO):
            hit = outer * (o_count == k).astype(jnp.int32)
            o[k] = jnp.where(hit == 1, i, o[k])
            o_ok[k] = o_ok[k] | hit
        q_count = q_count + inner
        o_count = o_count + outer
    last = N - 1
    q_par = [jnp.minimum(parent_ref[v], last) for v in q]
    o_up = [parent_ref[v] for v in o]
    o_par = [jnp.minimum(v, last) for v in o_up]
    o_over = [jnp.where(up < N, parent_ref[v], N) for up, v in zip(o_up, o_par)]
    o_grand = [jnp.minimum(v, last) for v in o_over]
    o_deep = [ok * (v < N).astype(jnp.int32) for ok, v in zip(o_ok, o_over)]
    o_slot = [q_ok[1] * (v == q[1]).astype(jnp.int32) for v in o_par]
    return dict(
        q=q, q_ok=q_ok, q_par=q_par, o=o, o_ok=o_ok, o_par=o_par, o_grand=o_grand, o_deep=o_deep, o_slot=o_slot
    )


def split(a):
    high = a.astype(BF16)
    return high, (a - high.astype(F32)).astype(BF16)


def dot3(a, b, transposed=False):
    dims = (((1,), (1 if transposed else 0,)), ((), ()))
    mul = lambda u, v: lax.dot_general(u, v, dims, preferred_element_type=F32)
    ah, al = a
    bh, bl = b
    return mul(ah, bh) + (mul(ah, bl) + mul(al, bh))


def masked_rows(block, first):
    rows = first + lax.broadcasted_iota(jnp.int32, block.shape, 0)
    cols = lax.axis_index(ROW) * H + lax.broadcasted_iota(jnp.int32, block.shape, 1)
    return jnp.where(rows >= cols, block, 0.0)


def pack_kernel(parent, marks, factor, q_out, o_out, held, sems):
    t = tree_of(parent)
    slots = [(t["q_par"][k], t["q"][k], t["q_ok"][k]) for k in range(NQ)]
    for j in range(NO):
        slots.append((t["o_par"][j], t["o"][j], t["o_ok"][j]))
        slots.append((t["o_grand"][j], t["o"][j], t["o_deep"][j]))
    copies = []
    for n, (up, node, _) in enumerate(slots):
        copies.append(pltpu.make_async_copy(factor.at[up, node], held.at[n], sems.at[n]))
        copies[-1].start()
    left = lax.broadcasted_iota(jnp.int32, (NARROW, H), 1) < H // 2
    for n, (up, node, ok) in enumerate(slots):
        copies[n].wait()
        first = (marks[node, 0, up] * ok).astype(F32)
        second = (marks[node, 1, up] * ok).astype(F32)
        block = held[n] * jnp.where(left, first, second)
        if n < NQ:
            q_out[n] = block
        else:
            o_out[(n - NQ) // 2, (n - NQ) % 2] = block


def q_part_kernel(parent, p0, p1, p2, p3, diag, out, strip, wide, sems):
    t = tree_of(parent)
    at = lax.axis_index("x")
    first = pl.multiple_of(at * STRIP, STRIP)
    copies = []
    for k in range(NQ):
        copies.append(pltpu.make_async_copy(diag.at[t["q_par"][k], pl.ds(first, STRIP)], strip.at[k], sems.at[k]))
        copies[-1].start()
    for step, piece in enumerate((p0, p1, p2, p3)):
        source = lax.rem(at + XS - step, XS)
        for k in range(NQ):
            wide[k, source] = piece[k]
    for k in range(NQ):
        copies[k].wait()
        left = split(masked_rows(strip[k], first))
        part = -dot3(left, split(wide[k].reshape(WIDE, H)), True)
        part = part.reshape(ZS, RS, FINE, WIDE)
        for r in range(RS):
            out[r, :, k] = part[:, r]


def rows_from(near, far, slot, rows):
    y_at, core_at = lax.axis_index("y"), lax.axis_index("core")
    for step in range(YS):
        y = lax.rem(y_at + YS - step, YS)
        for side, source in ((core_at, near), (1 - core_at, far)):
            first = pl.multiple_of((y * CS + side) * FINE, FINE)
            for z in range(ZS):
                rows[pl.ds(first, FINE), z * WIDE : (z + 1) * WIDE] = source[step, z, slot]


def q_solve_kernel(parent, near, far, diag, out, held, rows, sems):
    t = tree_of(parent)
    copies = []
    for k in range(NQ):
        copies.append(pltpu.make_async_copy(diag.at[t["q"][k]], held.at[k], sems.at[k]))
        copies[-1].start()
    for k in range(NQ):
        rows_from(near, far, k, rows)
        copies[k].wait()
        out[k] = dot3(split(rows[...]), split(masked_rows(held[k], 0)))


def near_part_kernel(parent, p0, p1, p2, p3, diag, near_out, base_out, wide_out, strip, wide, sems):
    t = tree_of(parent)
    at = lax.axis_index("x")
    first = pl.multiple_of(at * STRIP, STRIP)
    copies = []
    for j in range(NO):
        for e, node in enumerate((t["o_par"][j], t["o_grand"][j])):
            copies.append(pltpu.make_async_copy(diag.at[node, pl.ds(first, STRIP)], strip.at[j, e], sems.at[j, e]))
            copies[-1].start()
    for step, piece in enumerate((p0, p1, p2, p3)):
        source = lax.rem(at + XS - step, XS)
        for j in range(NO):
            for e in range(2):
                wide[j, e, source] = piece[j, e]
    for j in range(NO):
        for e in range(2):
            copies[2 * j + e].wait()
            left = split(masked_rows(strip[j, e], first))
            right = wide[j, e].reshape(WIDE, H)
            part = -dot3(left, split(right), True)
            if e == 0:
                part = part.reshape(ZS, RS, FINE, WIDE)
                for r in range(RS):
                    near_out[r, :, j] = part[:, r]
                wide_out[j] = right * t["o_deep"][j].astype(F32)
            else:
                base_out[j] = part


def far_part_kernel(parent, own, u1, u2, u3, d1, d2, d3, uh, dh, base, wide, out, tall):
    t = tree_of(parent)
    at = lax.axis_index("z")
    for step, piece in ((0, own), (1, u1), (2, u2), (3, u3), (-1, d1), (-2, d2), (-3, d3)):
        source = lax.rem(at + ZS - step, ZS)
        for k in range(NQ):
            tall[k, source] = piece[k]
    source = lax.rem(at + ZS // 2, ZS)
    tall[0, source] = uh[0]
    tall[1, source] = dh[0]
    for j in range(NO):
        left = split(tall[t["o_slot"][j]].reshape(STRIP, H))
        part = base[j] - dot3(left, split(wide[j]), True)
        part = part.reshape(ZS, RS, FINE, WIDE)
        for r in range(RS):
            out[r, :, j] = part[:, r]


def near_solve_kernel(parent, near, far, diag, q_done, load, mean_out, square_out, held, own, rows, sems, own_sems):
    t = tree_of(parent)
    first = pl.multiple_of(lax.axis_index("x") * STRIP + lax.axis_index("z") * CHUNK, CHUNK)
    own_copies, copies = [], []
    for s in range(N):
        own_copies.append(pltpu.make_async_copy(diag.at[s, pl.ds(first, CHUNK)], own.at[s], own_sems.at[s]))
        own_copies[-1].start()
    for j in range(NO):
        copies.append(pltpu.make_async_copy(diag.at[t["o"][j]], held.at[j], sems.at[j]))
        copies[-1].start()
    square_out[...] = jnp.zeros_like(square_out)
    for s in range(N):
        own_copies[s].wait()
        block = masked_rows(own[s], first)
        mean_out[s] = dot3(split(load[s]), split(block))
        square_out[s] = jnp.sum(block * block, axis=0, keepdims=True)
    for k in range(NQ):
        node = t["q"][k]
        done = q_done[k]
        mean_out[node] += dot3(split(load[t["q_par"][k]]), split(done))
        square_out[node] += jnp.sum(done * done, axis=0, keepdims=True)
    for j in range(NO):
        node = t["o"][j]
        rows_from(near, far, j, rows)
        copies[j].wait()
        done = dot3(split(rows[...]), split(masked_rows(held[j], 0)))
        mean_out[node] += dot3(split(load[t["o_par"][j]]), split(done))
        square_out[node] += jnp.sum(done * done, axis=0, keepdims=True)


def far_solve_kernel(parent, near, far, diag, mean_in, square_in, load, out, held, mean, square, rows, sems):
    t = tree_of(parent)
    copies = []
    for j in range(NO):
        copies.append(pltpu.make_async_copy(diag.at[t["o"][j]], held.at[j], sems.at[j]))
        copies[-1].start()
    mean[...] = mean_in[...]
    square[...] = square_in[...]
    for j in range(NO):
        node = t["o"][j]
        rows_from(near, far, j, rows)
        copies[j].wait()
        done = dot3(split(rows[...]), split(masked_rows(held[j], 0)))
        mean[node] += dot3(split(load[t["o_grand"][j]]), split(done))
        square[node] += jnp.sum(done * done, axis=0, keepdims=True)
    each = RHS // XS
    for x in range(XS):
        for s in range(N):
            out[x, s] = mean[s, x * each : (x + 1) * each]
        out[x, N] = jnp.zeros((each, H), F32)
        for s in range(N):
            out[x, N, s : s + 1] = square[s]


def turn_kernel(parts, out):
    total = parts[0]
    for x in range(1, XS):
        total = total + parts[x]
    each = RHS // (XS * ZS)
    for z in range(ZS):
        out[z, 2 * N : 3 * N] = total[N, :N]
        out[z, 3 * N :] = jnp.zeros((24 - 3 * N, H), F32)
        for s in range(N):
            out[z, each * s : each * (s + 1)] = total[s, each * z : each * (z + 1)]


def shifted(array, axis, step):
    size = lax.axis_size(axis)
    return lax.ppermute(array, axis, [(i, (i + step) % size) for i in range(size)])


def by_distance(array, axis):
    return [array] + [shifted(array, axis, step) for step in range(1, lax.axis_size(axis))]


def row_gathered(array):
    near = jnp.stack(by_distance(array, "y"))
    return near, shifted(near, "core", 1)


def summed_rows(partial):
    own = jnp.sum(lax.all_to_all(partial, ROW, 0, 0, tiled=True), axis=0)
    return lax.all_to_all(own, "z", 0, 0, tiled=True)


def rhs_load(post):
    rhs = post.shape[2]
    core, y_at = lax.axis_index("core"), lax.axis_index("y")
    thin = jnp.transpose(post, (0, 2, 1)).reshape(N * rhs, H)
    near, far = row_gathered(thin)
    turn = lambda a: jnp.roll(a[::-1], y_at + 1, axis=0)
    near, far = turn(near), turn(far)
    both = jnp.stack([jnp.where(core == 0, near, far), jnp.where(core == 0, far, near)], axis=1)
    tall = jnp.transpose(both.reshape(RS, N * rhs, H), (1, 0, 2)).reshape(N * rhs, XS, STRIP)
    by_x = lax.all_to_all(tall, "x", 1, 0, tiled=False)
    by_z = lax.all_to_all(by_x.reshape(XS, N * rhs, ZS, CHUNK), "z", 2, 0, tiled=False)
    load = by_z.reshape(ZS, XS, N, rhs, CHUNK)
    return jnp.transpose(load, (2, 1, 0, 3, 4)).reshape(N, RHS, CHUNK)


def body(factor, diag, structure, parent, post):
    dma = pltpu.SemaphoreType.DMA
    blocks = jnp.transpose(factor, (0, 2, 3, 1))
    marks = jnp.transpose(structure, (0, 2, 1))
    q_pack, o_pack = call(
        pack_kernel,
        (shape(NQ, NARROW, H), shape(NO, 2, NARROW, H)),
        [SMEM, SMEM, HBM],
        [pltpu.VMEM((NQ + 2 * NO, NARROW, H), F32), dma((NQ + 2 * NO,))],
    )(parent, marks, blocks)
    q_pieces = by_distance(q_pack, "x")
    o_pieces = by_distance(o_pack, "x")

    q_part = call(
        q_part_kernel,
        shape(RS, ZS, NQ, FINE, WIDE),
        [SMEM, VMEM, VMEM, VMEM, VMEM, HBM],
        [pltpu.VMEM((NQ, STRIP, H), F32), pltpu.VMEM((NQ, XS, NARROW, H), F32), dma((NQ,))],
    )(parent, *q_pieces, diag)
    q_near, q_far = row_gathered(summed_rows(q_part))
    q_done = call(
        q_solve_kernel,
        shape(NQ, CHUNK, H),
        [SMEM, VMEM, VMEM, HBM],
        [pltpu.VMEM((NQ, W, H), F32), pltpu.VMEM((CHUNK, W), F32), dma((NQ,))],
    )(parent, q_near, q_far, diag)

    near_part, base, o_wide = call(
        near_part_kernel,
        (shape(RS, ZS, NO, FINE, WIDE), shape(NO, STRIP, WIDE), shape(NO, WIDE, H)),
        [SMEM, VMEM, VMEM, VMEM, VMEM, HBM],
        [pltpu.VMEM((NO, 2, STRIP, H), F32), pltpu.VMEM((NO, 2, XS, NARROW, H), F32), dma((NO, 2))],
    )(parent, *o_pieces, diag)
    near_near, near_far = row_gathered(summed_rows(near_part))

    up, down = [q_done], [q_done]
    for _ in range(ZS // 2 - 1):
        up.append(shifted(up[-1], "z", 1))
        down.append(shifted(down[-1], "z", ZS - 1))
    up_half = shifted(up[-1][:1], "z", 1)
    down_half = shifted(down[-1][1:], "z", ZS - 1)
    far_part = call(
        far_part_kernel,
        shape(RS, ZS, NO, FINE, WIDE),
        [SMEM] + [VMEM] * 11,
        [pltpu.VMEM((NQ, ZS, CHUNK, H), F32)],
    )(parent, *up, *down[1:], up_half, down_half, base, o_wide)
    far_near, far_far = row_gathered(summed_rows(far_part))

    load = rhs_load(post)
    mean, square = call(
        near_solve_kernel,
        (shape(N, RHS, H), shape(N, 1, H)),
        [SMEM, VMEM, VMEM, HBM, VMEM, VMEM],
        [
            pltpu.VMEM((NO, W, H), F32),
            pltpu.VMEM((N, CHUNK, H), F32),
            pltpu.VMEM((CHUNK, W), F32),
            dma((NO,)),
            dma((N,)),
        ],
    )(parent, near_near, near_far, diag, q_done, load)
    packed = call(
        far_solve_kernel,
        shape(XS, N + 1, RHS // XS, H),
        [SMEM, VMEM, VMEM, HBM, VMEM, VMEM, VMEM],
        [
            pltpu.VMEM((NO, W, H), F32),
            pltpu.VMEM((N, RHS, H), F32),
            pltpu.VMEM((N, 1, H), F32),
            pltpu.VMEM((CHUNK, W), F32),
            dma((NO,)),
        ],
    )(parent, far_near, far_far, diag, mean, square, load)
    packed = lax.all_to_all(packed, "x", 0, 0, tiled=True)
    packed = call(turn_kernel, shape(ZS, 24, H), [VMEM], [])(packed)
    total = jnp.sum(lax.all_to_all(packed, "z", 0, 0, tiled=True), axis=0)
    mean_x = jnp.transpose(total[: 2 * N].reshape(N, 2, H), (0, 2, 1))
    return mean_x, total[2 * N : 3 * N]


def solution(mesh):
    finer = Mesh(mesh.devices.reshape(YS, CS, ZS, XS), (*ROW, *COL))
    placed = (
        P(None, ROW, None, COL),
        P(None, None, ROW),
        P(None, None, ROW),
        P(),
        P(None, ROW, COL),
    )
    return jax.shard_map(
        body,
        mesh=finer,
        in_specs=placed,
        out_specs=(P(None, ROW, COL), P(None, ROW)),
        check_vma=False,
    )
```

```python
import functools

import jax
import jax.numpy as jnp
from jax import lax
from jax.experimental import pallas as pl
from jax.experimental.pallas import tpu as pltpu
from jax.sharding import Mesh
from jax.sharding import PartitionSpec as P

ROW = ("y", "core")
COL = ("z", "x")
F32 = jnp.float32
BF16 = jnp.bfloat16

N = 6
W = 2048
H = 256
YS, CS, ZS, XS = 4, 2, 8, 4
RS = YS * CS
NARROW = W // (ZS * XS)
WIDE = NARROW * XS
STRIP = W // XS
CHUNK = STRIP // ZS
FINE = CHUNK // RS
RUN = STRIP // RS
NQ, NO = 2, 4
RHS = 64

SMEM = pl.BlockSpec(memory_space=pltpu.SMEM)
VMEM = pl.BlockSpec(memory_space=pltpu.VMEM)
HBM = pl.BlockSpec(memory_space=pl.ANY)


def call(kernel, outs, in_specs, scratch, flops=10**9):
    return pl.pallas_call(
        kernel,
        out_shape=outs,
        cost_estimate=pl.CostEstimate(flops=flops, bytes_accessed=10**7, transcendentals=0),
        in_specs=in_specs,
        out_specs=jax.tree.map(lambda _: VMEM, outs),
        scratch_shapes=scratch,
        compiler_params=pltpu.CompilerParams(vmem_limit_bytes=56 * 1024 * 1024),
    )


def shape(*dims):
    return jax.ShapeDtypeStruct(dims, F32)


def tree_of(parent_ref):
    par = [parent_ref[i] for i in range(N)]
    zero = jnp.int32(0)
    q, q_ok, o, o_ok = [zero] * NQ, [zero] * NQ, [zero] * NO, [zero] * NO
    q_count = o_count = zero
    for i in range(N):
        has_parent = (par[i] < N).astype(jnp.int32)
        has_child = zero
        for s in range(i):
            has_child = has_child | (par[s] == i).astype(jnp.int32)
        inner = has_parent * has_child
        outer = has_parent * (1 - has_child)
        for k in range(NQ):
            hit = inner * (q_count == k).astype(jnp.int32)
            q[k] = jnp.where(hit == 1, i, q[k])
            q_ok[k] = q_ok[k] | hit
        for k in range(NO):
            hit = outer * (o_count == k).astype(jnp.int32)
            o[k] = jnp.where(hit == 1, i, o[k])
            o_ok[k] = o_ok[k] | hit
        q_count = q_count + inner
        o_count = o_count + outer
    last = N - 1
    q_par = [jnp.minimum(parent_ref[v], last) for v in q]
    o_up = [parent_ref[v] for v in o]
    o_par = [jnp.minimum(v, last) for v in o_up]
    o_over = [jnp.where(up < N, parent_ref[v], N) for up, v in zip(o_up, o_par)]
    o_grand = [jnp.minimum(v, last) for v in o_over]
    o_deep = [ok * (v < N).astype(jnp.int32) for ok, v in zip(o_ok, o_over)]
    o_slot = [q_ok[1] * (v == q[1]).astype(jnp.int32) for v in o_par]
    return dict(
        q=q, q_ok=q_ok, q_par=q_par, o=o, o_ok=o_ok, o_par=o_par, o_grand=o_grand, o_deep=o_deep, o_slot=o_slot
    )


def split(a):
    high = a.astype(BF16)
    return high, (a - high.astype(F32)).astype(BF16)


def dot3(a, b, transposed=False):
    dims = (((1,), (1 if transposed else 0,)), ((), ()))
    mul = lambda u, v: lax.dot_general(u, v, dims, preferred_element_type=F32)
    ah, al = a
    bh, bl = b
    return mul(ah, bh) + (mul(ah, bl) + mul(al, bh))


def masked_rows(block, first=0, run=W):
    at = lax.broadcasted_iota(jnp.int32, block.shape, 0)
    rows = first + at if run == W else first + (at // run) * H + at % run
    cols = lax.axis_index(ROW) * H + lax.broadcasted_iota(jnp.int32, block.shape, 1)
    return jnp.where(rows >= cols, block, 0.0)


def put_row_parts(part, index, mine, other, parts):
    core = lax.axis_index("core")
    parts[...] = part.reshape(YS, CS, ZS, FINE, WIDE)
    mine[:, :, index] = parts[:, core]
    other[:, :, index] = parts[:, 1 - core]


def pack_kernel(parent, marks, factor, thin, q_out, o_out, held, sems):
    t = tree_of(parent)
    slots = [(t["q_par"][k], t["q"][k], t["q_ok"][k]) for k in range(NQ)]
    for j in range(NO):
        slots.append((t["o_par"][j], t["o"][j], t["o_ok"][j]))
        slots.append((t["o_grand"][j], t["o"][j], t["o_deep"][j]))
    copies = []
    for n, (up, node, _) in enumerate(slots):
        copies.append(pltpu.make_async_copy(factor.at[up, node], held.at[n], sems.at[n]))
        copies[-1].start()
    left = lax.broadcasted_iota(jnp.int32, (NARROW, H), 1) < H // 2
    q_out[NQ * NARROW : NQ * NARROW + 2 * N] = thin[...]
    q_out[NQ * NARROW + 2 * N :] = jnp.zeros((16 - 2 * N, H), F32)
    for n, (up, node, ok) in enumerate(slots):
        copies[n].wait()
        first = (marks[node, 0, up] * ok).astype(F32)
        second = (marks[node, 1, up] * ok).astype(F32)
        block = held[n] * jnp.where(left, first, second)
        if n < NQ:
            q_out[n * NARROW : (n + 1) * NARROW] = block
        else:
            o_out[(n - NQ) // 2, (n - NQ) % 2] = block


def q_part_kernel(parent, p0, p1, p2, p3, diag, mine, other, rhs_out, strip, wide, parts, thin, tall, sems):
    t = tree_of(parent)
    at = lax.axis_index("x")
    copies = []
    for k in range(NQ):
        copies.append(pltpu.make_async_copy(diag.at[t["q_par"][k], :, at], strip.at[k], sems.at[k]))
        copies[-1].start()
    thin[...] = jnp.zeros_like(thin)
    for step, piece in enumerate((p0, p1, p2, p3)):
        source = lax.rem(at + XS - step, XS)
        for k in range(NQ):
            wide[k, source] = piece[k * NARROW : (k + 1) * NARROW]
        thin[pl.ds(pl.multiple_of(source * 16, 16), 16)] = piece[NQ * NARROW :]
    tall[...] = thin[...].T
    rhs_out[...] = tall[pl.ds(pl.multiple_of(at * RUN, RUN), RUN)].reshape(ZS, FINE, 128)
    for k in range(NQ):
        copies[k].wait()
        left = split(masked_rows(strip[k].reshape(STRIP, H), at * RUN, RUN))
        part = -dot3(left, split(wide[k].reshape(WIDE, H)), True)
        put_row_parts(part, k, mine, other, parts)


def rows_from(near, far, slot, rows):
    y_at, core_at = lax.axis_index("y"), lax.axis_index("core")
    for step in range(YS):
        y = lax.rem(y_at + YS - step, YS)
        for side, source in ((core_at, near), (1 - core_at, far)):
            first = pl.multiple_of((y * CS + side) * FINE, FINE)
            for z in range(ZS):
                rows[pl.ds(first, FINE), z * WIDE : (z + 1) * WIDE] = source[step, z, slot]


def q_solve_kernel(parent, near, far, diag, out, held, rows, sems):
    t = tree_of(parent)
    copies = []
    for k in range(NQ):
        copies.append(pltpu.make_async_copy(diag.at[t["q"][k]], held.at[k], sems.at[k]))
        copies[-1].start()
    for k in range(NQ):
        rows_from(near, far, k, rows)
        copies[k].wait()
        out[k] = dot3(split(rows[...]), split(masked_rows(held[k])))


def near_part_kernel(parent, p0, p1, p2, p3, diag, mine, other, base_out, wide_out, strip, wide, parts, sems):
    t = tree_of(parent)
    at = lax.axis_index("x")
    copies = []
    for j in range(NO):
        for e, node in enumerate((t["o_par"][j], t["o_grand"][j])):
            copies.append(pltpu.make_async_copy(diag.at[node, :, at], strip.at[j, e], sems.at[j, e]))
            copies[-1].start()
    for step, piece in enumerate((p0, p1, p2, p3)):
        source = lax.rem(at + XS - step, XS)
        for j in range(NO):
            for e in range(2):
                wide[j, e, source] = piece[j, e]
    for j in range(NO):
        for e in range(2):
            copies[2 * j + e].wait()
            left = split(masked_rows(strip[j, e].reshape(STRIP, H), at * RUN, RUN))
            right = wide[j, e].reshape(WIDE, H)
            part = -dot3(left, split(right), True)
            if e == 0:
                put_row_parts(part, j, mine, other, parts)
                wide_out[j] = right * t["o_deep"][j].astype(F32)
            else:
                base_out[j] = part


def far_part_kernel(parent, own, u1, u2, u3, d1, d2, d3, uh, dh, base, wide, mine, other, tall, parts):
    t = tree_of(parent)
    at = lax.axis_index("z")
    for step, piece in ((0, own), (1, u1), (2, u2), (3, u3), (-1, d1), (-2, d2), (-3, d3)):
        source = lax.rem(at + ZS - step, ZS)
        for k in range(NQ):
            tall[k, :, source] = piece[k].reshape(RS, FINE, H)
    source = lax.rem(at + ZS // 2, ZS)
    tall[0, :, source] = uh[0].reshape(RS, FINE, H)
    tall[1, :, source] = dh[0].reshape(RS, FINE, H)
    for j in range(NO):
        left = split(tall[t["o_slot"][j]].reshape(STRIP, H))
        part = base[j] - dot3(left, split(wide[j]), True)
        put_row_parts(part, j, mine, other, parts)


def near_solve_kernel(
    parent, near, far, diag, fine, q_done, q_near, q_far,
    mean_out, square_out, load, held, own, rows, thin, sems, own_sems,
):
    t = tree_of(parent)
    x_at, z_at = lax.axis_index("x"), lax.axis_index("z")
    own_copies, copies = [], []
    for s in range(N):
        own_copies.append(pltpu.make_async_copy(fine.at[s, :, x_at, z_at], own.at[s], own_sems.at[s]))
        own_copies[-1].start()
    for j in range(NO):
        copies.append(pltpu.make_async_copy(diag.at[t["o"][j]], held.at[j], sems.at[j]))
        copies[-1].start()
    y_at, core_at = lax.axis_index("y"), lax.axis_index("core")
    for z in range(ZS):
        for step in range(YS):
            y = lax.rem(y_at + YS - step, YS)
            for side, source in ((core_at, q_near), (1 - core_at, q_far)):
                at = pl.multiple_of((y * CS + side) * FINE, FINE)
                thin[pl.ds(at, FINE)] = source[step, z, NQ][:, :128]
        flat = thin[...].T
        for x in range(XS):
            for s in range(N):
                to = 16 * x + 2 * z
                load[s, to : to + 2] = flat[16 * x + 2 * s : 16 * x + 2 * s + 2]
    for s in range(N):
        own_copies[s].wait()
        block = masked_rows(own[s].reshape(CHUNK, H), x_at * RUN + z_at * FINE, FINE)
        mean_out[s] = dot3(split(load[s]), split(block))
        square_out[s] = jnp.sum(block * block, axis=0, keepdims=True)
    for k in range(NQ):
        node = t["q"][k]
        done = q_done[k]
        mean_out[node] += dot3(split(load[t["q_par"][k]]), split(done))
        square_out[node] += jnp.sum(done * done, axis=0, keepdims=True)
    for j in range(NO):
        node = t["o"][j]
        rows_from(near, far, j, rows)
        copies[j].wait()
        done = dot3(split(rows[...]), split(masked_rows(held[j])))
        mean_out[node] += dot3(split(load[t["o_par"][j]]), split(done))
        square_out[node] += jnp.sum(done * done, axis=0, keepdims=True)


def far_solve_kernel(parent, near, far, diag, mean_in, square_in, load, out, held, mean, square, rows, sems):
    t = tree_of(parent)
    copies = []
    for j in range(NO):
        copies.append(pltpu.make_async_copy(diag.at[t["o"][j]], held.at[j], sems.at[j]))
        copies[-1].start()
    mean[...] = mean_in[...]
    square[...] = square_in[...]
    for j in range(NO):
        node = t["o"][j]
        rows_from(near, far, j, rows)
        copies[j].wait()
        done = dot3(split(rows[...]), split(masked_rows(held[j])))
        mean[node] += dot3(split(load[t["o_grand"][j]]), split(done))
        square[node] += jnp.sum(done * done, axis=0, keepdims=True)
    each = RHS // XS
    for x in range(XS):
        for s in range(N):
            out[x, s] = mean[s, x * each : (x + 1) * each]
        out[x, N] = jnp.zeros((each, H), F32)
        for s in range(N):
            out[x, N, s : s + 1] = square[s]


def turn_kernel(parts, out):
    total = parts[0]
    for x in range(1, XS):
        total = total + parts[x]
    each = RHS // (XS * ZS)
    for z in range(ZS):
        out[z, 2 * N : 3 * N] = total[N, :N]
        out[z, 3 * N :] = jnp.zeros((24 - 3 * N, H), F32)
        for s in range(N):
            out[z, each * s : each * (s + 1)] = total[s, each * z : each * (z + 1)]


def shifted(array, axis, step):
    size = lax.axis_size(axis)
    return lax.ppermute(array, axis, [(i, (i + step) % size) for i in range(size)])


def by_distance(array, axis):
    return [array] + [shifted(array, axis, step) for step in range(1, lax.axis_size(axis))]


def row_gathered(array):
    near = jnp.stack(by_distance(array, "y"))
    return near, shifted(near, "core", 1)


def summed_rows(mine, other):
    paired = mine + shifted(other, "core", 1)
    return jnp.sum(lax.all_to_all(paired, "y", 0, 0, tiled=True), axis=0)


def turned(own):
    return lax.all_to_all(own, "z", 0, 0, tiled=True)


def body(factor, diag, structure, parent, post):
    dma = pltpu.SemaphoreType.DMA
    blocks = jnp.transpose(factor, (0, 2, 3, 1))
    marks = jnp.transpose(structure, (0, 2, 1))
    thin = jnp.transpose(post, (0, 2, 1)).reshape(2 * N, H)
    runs = diag.reshape(N, RS, XS, RUN, H)
    fine = diag.reshape(N, RS, XS, ZS, FINE, H)
    q_pack, o_pack = call(
        pack_kernel,
        (shape(NQ * NARROW + 16, H), shape(NO, 2, NARROW, H)),
        [SMEM, SMEM, HBM, VMEM],
        [pltpu.VMEM((NQ + 2 * NO, NARROW, H), F32), dma((NQ + 2 * NO,))],
    )(parent, marks, blocks, thin)
    q_pieces = by_distance(q_pack, "x")
    o_pieces = by_distance(o_pack, "x")

    def parts_of(n):
        return (shape(YS, ZS, n, FINE, WIDE), shape(YS, ZS, n, FINE, WIDE))

    parts = pltpu.VMEM((YS, CS, ZS, FINE, WIDE), F32)
    q_mine, q_other, q_rhs = call(
        q_part_kernel,
        (*parts_of(NQ), shape(ZS, FINE, 128)),
        [SMEM, VMEM, VMEM, VMEM, VMEM, HBM],
        [
            pltpu.VMEM((NQ, RS, RUN, H), F32),
            pltpu.VMEM((NQ, XS, NARROW, H), F32),
            parts,
            pltpu.VMEM((128, H), F32),
            pltpu.VMEM((H, 128), F32),
            dma((NQ,)),
        ],
    )(parent, *q_pieces, runs)
    q_own = summed_rows(q_mine, q_other)
    q_rhs = jnp.pad(q_rhs[:, None], ((0, 0), (0, 0), (0, 0), (0, H - 128)))
    q_near, q_far = row_gathered(turned(jnp.concatenate([q_own, q_rhs], axis=1)))
    q_done = call(
        q_solve_kernel,
        shape(NQ, CHUNK, H),
        [SMEM, VMEM, VMEM, HBM],
        [pltpu.VMEM((NQ, W, H), F32), pltpu.VMEM((CHUNK, W), F32), dma((NQ,))],
    )(parent, q_near, q_far, diag)

    near_mine, near_other, base, o_wide = call(
        near_part_kernel,
        (*parts_of(NO), shape(NO, STRIP, WIDE), shape(NO, WIDE, H)),
        [SMEM, VMEM, VMEM, VMEM, VMEM, HBM],
        [pltpu.VMEM((NO, 2, RS, RUN, H), F32), pltpu.VMEM((NO, 2, XS, NARROW, H), F32), parts, dma((NO, 2))],
    )(parent, *o_pieces, runs)
    near_mine, near_other, q_done = lax.optimization_barrier((near_mine, near_other, q_done))

    up, down = [q_done], [q_done]
    for _ in range(ZS // 2 - 1):
        up.append(shifted(up[-1], "z", 1))
        down.append(shifted(down[-1], "z", ZS - 1))
    up_half = shifted(up[-1][:1], "z", 1)
    down_half = shifted(down[-1][1:], "z", ZS - 1)
    near_own = summed_rows(near_mine, near_other)
    far_mine, far_other = call(
        far_part_kernel,
        parts_of(NO),
        [SMEM] + [VMEM] * 11,
        [pltpu.VMEM((NQ, RS, ZS, FINE, H), F32), parts],
    )(parent, *up, *down[1:], up_half, down_half, base, o_wide)
    near_turned = turned(near_own)
    far_own = summed_rows(far_mine, far_other)
    near_turned, far_own = lax.optimization_barrier((near_turned, far_own))
    near_near, near_far = row_gathered(near_turned)
    far_near, far_far = row_gathered(turned(far_own))

    mean, square, load = call(
        near_solve_kernel,
        (shape(N, RHS, H), shape(N, 1, H), shape(N, RHS, CHUNK)),
        [SMEM, VMEM, VMEM, HBM, HBM, VMEM, VMEM, VMEM],
        [
            pltpu.VMEM((NO, W, H), F32),
            pltpu.VMEM((N, RS, FINE, H), F32),
            pltpu.VMEM((CHUNK, W), F32),
            pltpu.VMEM((CHUNK, 128), F32),
            dma((NO,)),
            dma((N,)),
        ],
    )(parent, near_near, near_far, diag, fine, q_done, q_near, q_far)
    packed = call(
        far_solve_kernel,
        shape(XS, N + 1, RHS // XS, H),
        [SMEM, VMEM, VMEM, HBM, VMEM, VMEM, VMEM],
        [
            pltpu.VMEM((NO, W, H), F32),
            pltpu.VMEM((N, RHS, H), F32),
            pltpu.VMEM((N, 1, H), F32),
            pltpu.VMEM((CHUNK, W), F32),
            dma((NO,)),
        ],
    )(parent, far_near, far_far, diag, mean, square, load)
    packed = lax.all_to_all(packed, "x", 0, 0, tiled=True)
    packed = call(turn_kernel, shape(ZS, 24, H), [VMEM], [])(packed)
    total = jnp.sum(lax.all_to_all(packed, "z", 0, 0, tiled=True), axis=0)
    mean_x = jnp.transpose(total[: 2 * N].reshape(N, 2, H), (0, 2, 1))
    return mean_x, total[2 * N : 3 * N]


def solution(mesh):
    finer = Mesh(mesh.devices.reshape(YS, CS, ZS, XS), (*ROW, *COL))
    placed = (
        P(None, ROW, None, COL),
        P(None, None, ROW),
        P(None, None, ROW),
        P(),
        P(None, ROW, COL),
    )
    return jax.shard_map(
        body,
        mesh=finer,
        in_specs=placed,
        out_specs=(P(None, ROW, COL), P(None, ROW)),
        check_vma=False,
    )
```

```python
import functools

import jax
import jax.numpy as jnp
from jax import lax
from jax.experimental import pallas as pl
from jax.experimental.pallas import tpu as pltpu
from jax.sharding import Mesh
from jax.sharding import PartitionSpec as P

ROW = ("y", "core")
COL = ("z", "x")
F32 = jnp.float32
BF16 = jnp.bfloat16

N = 6
W = 2048
H = 256
YS, CS, ZS, XS = 4, 2, 8, 4
RS = YS * CS
NARROW = W // (ZS * XS)
WIDE = NARROW * XS
STRIP = W // XS
CHUNK = STRIP // ZS
FINE = CHUNK // RS
RUN = STRIP // RS
NQ, NO = 2, 4
RHS = 64

SMEM = pl.BlockSpec(memory_space=pltpu.SMEM)
VMEM = pl.BlockSpec(memory_space=pltpu.VMEM)
HBM = pl.BlockSpec(memory_space=pl.ANY)


def call(kernel, outs, in_specs, scratch, mib, flops=10**9):
    return pl.pallas_call(
        kernel,
        out_shape=outs,
        cost_estimate=pl.CostEstimate(flops=flops, bytes_accessed=10**7, transcendentals=0),
        in_specs=in_specs,
        out_specs=jax.tree.map(lambda _: VMEM, outs),
        scratch_shapes=scratch,
        compiler_params=pltpu.CompilerParams(vmem_limit_bytes=mib * 1024 * 1024),
    )


def shape(*dims):
    return jax.ShapeDtypeStruct(dims, F32)


def tree_of(parent_ref):
    par = [parent_ref[i] for i in range(N)]
    zero = jnp.int32(0)
    q, q_ok, o, o_ok = [zero] * NQ, [zero] * NQ, [zero] * NO, [zero] * NO
    q_count = o_count = zero
    for i in range(N):
        has_parent = (par[i] < N).astype(jnp.int32)
        has_child = zero
        for s in range(i):
            has_child = has_child | (par[s] == i).astype(jnp.int32)
        inner = has_parent * has_child
        outer = has_parent * (1 - has_child)
        for k in range(NQ):
            hit = inner * (q_count == k).astype(jnp.int32)
            q[k] = jnp.where(hit == 1, i, q[k])
            q_ok[k] = q_ok[k] | hit
        for k in range(NO):
            hit = outer * (o_count == k).astype(jnp.int32)
            o[k] = jnp.where(hit == 1, i, o[k])
            o_ok[k] = o_ok[k] | hit
        q_count = q_count + inner
        o_count = o_count + outer
    last = N - 1
    q_par = [jnp.minimum(parent_ref[v], last) for v in q]
    o_up = [parent_ref[v] for v in o]
    o_par = [jnp.minimum(v, last) for v in o_up]
    o_over = [jnp.where(up < N, parent_ref[v], N) for up, v in zip(o_up, o_par)]
    o_grand = [jnp.minimum(v, last) for v in o_over]
    o_deep = [ok * (v < N).astype(jnp.int32) for ok, v in zip(o_ok, o_over)]
    o_slot = [q_ok[1] * (v == q[1]).astype(jnp.int32) for v in o_par]
    return dict(
        q=q, q_ok=q_ok, q_par=q_par, o=o, o_ok=o_ok, o_par=o_par, o_grand=o_grand, o_deep=o_deep, o_slot=o_slot
    )


def split(a):
    high = a.astype(BF16)
    return high, (a - high.astype(F32)).astype(BF16)


def dot3(a, b, transposed=False):
    dims = (((1,), (1 if transposed else 0,)), ((), ()))
    mul = lambda u, v: lax.dot_general(u, v, dims, preferred_element_type=F32)
    ah, al = a
    bh, bl = b
    return mul(ah, bh) + (mul(ah, bl) + mul(al, bh))


def masked_rows(block, first=0, run=W):
    at = lax.broadcasted_iota(jnp.int32, block.shape, 0)
    rows = first + at if run == W else first + (at // run) * H + at % run
    cols = lax.axis_index(ROW) * H + lax.broadcasted_iota(jnp.int32, block.shape, 1)
    return jnp.where(rows >= cols, block, 0.0)


def put_row_parts(part, index, mine, other, parts):
    core = lax.axis_index("core")
    parts[...] = part.reshape(YS, CS, ZS, FINE, WIDE)
    mine[:, :, index] = parts[:, core]
    other[:, :, index] = parts[:, 1 - core]


def pack_kernel(parent, marks, factor, thin, q_out, o_out, held, sems):
    t = tree_of(parent)
    slots = [(t["q_par"][k], t["q"][k], t["q_ok"][k]) for k in range(NQ)]
    for j in range(NO):
        slots.append((t["o_par"][j], t["o"][j], t["o_ok"][j]))
        slots.append((t["o_grand"][j], t["o"][j], t["o_deep"][j]))
    copies = []
    for n, (up, node, _) in enumerate(slots):
        copies.append(pltpu.make_async_copy(factor.at[up, node], held.at[n], sems.at[n]))
        copies[-1].start()
    left = lax.broadcasted_iota(jnp.int32, (NARROW, H), 1) < H // 2
    q_out[NQ * NARROW : NQ * NARROW + 2 * N] = thin[...]
    q_out[NQ * NARROW + 2 * N :] = jnp.zeros((16 - 2 * N, H), F32)
    for n, (up, node, ok) in enumerate(slots):
        copies[n].wait()
        first = (marks[node, 0, up] * ok).astype(F32)
        second = (marks[node, 1, up] * ok).astype(F32)
        block = held[n] * jnp.where(left, first, second)
        if n < NQ:
            q_out[n * NARROW : (n + 1) * NARROW] = block
        else:
            o_out[(n - NQ) // 2, (n - NQ) % 2] = block


def q_part_kernel(parent, p0, p1, p2, p3, diag, mine, other, rhs_out, strip, wide, parts, thin, tall, sems):
    t = tree_of(parent)
    at = lax.axis_index("x")
    copies = []
    for k in range(NQ):
        copies.append(pltpu.make_async_copy(diag.at[t["q_par"][k], :, at], strip.at[k], sems.at[k]))
        copies[-1].start()
    thin[...] = jnp.zeros_like(thin)
    for step, piece in enumerate((p0, p1, p2, p3)):
        source = lax.rem(at + XS - step, XS)
        for k in range(NQ):
            wide[k, source] = piece[k * NARROW : (k + 1) * NARROW]
        thin[pl.ds(pl.multiple_of(source * 16, 16), 16)] = piece[NQ * NARROW :]
    tall[...] = thin[...].T
    rhs_out[...] = tall[pl.ds(pl.multiple_of(at * RUN, RUN), RUN)].reshape(ZS, FINE, 128)
    for k in range(NQ):
        copies[k].wait()
        left = split(masked_rows(strip[k].reshape(STRIP, H), at * RUN, RUN))
        part = -dot3(left, split(wide[k].reshape(WIDE, H)), True)
        put_row_parts(part, k, mine, other, parts)


def rows_from(pieces, slot, rows):
    y_at, core_at = lax.axis_index("y"), lax.axis_index("core")
    for step in range(YS):
        y = lax.rem(y_at + YS - step, YS)
        for side, source in ((core_at, pieces[step]), (1 - core_at, pieces[YS + step])):
            first = pl.multiple_of((y * CS + side) * FINE, FINE)
            for z in range(ZS):
                rows[pl.ds(first, FINE), z * WIDE : (z + 1) * WIDE] = source[z, slot]


def q_solve_kernel(parent, *refs):
    pieces, (diag, out, held, rows, sems) = refs[: 2 * YS], refs[2 * YS :]
    t = tree_of(parent)
    copies = []
    for k in range(NQ):
        copies.append(pltpu.make_async_copy(diag.at[t["q"][k]], held.at[k], sems.at[k]))
        copies[-1].start()
    for k in range(NQ):
        rows_from(pieces, k, rows)
        copies[k].wait()
        out[k] = dot3(split(rows[...]), split(masked_rows(held[k])))


def near_part_kernel(parent, p0, p1, p2, p3, diag, mine, other, base_out, wide_out, strip, wide, parts, sems):
    t = tree_of(parent)
    at = lax.axis_index("x")
    copies = []
    for j in range(NO):
        for e, node in enumerate((t["o_par"][j], t["o_grand"][j])):
            copies.append(pltpu.make_async_copy(diag.at[node, :, at], strip.at[j, e], sems.at[j, e]))
            copies[-1].start()
    for step, piece in enumerate((p0, p1, p2, p3)):
        source = lax.rem(at + XS - step, XS)
        for j in range(NO):
            for e in range(2):
                wide[j, e, source] = piece[j, e]
    for j in range(NO):
        for e in range(2):
            copies[2 * j + e].wait()
            left = split(masked_rows(strip[j, e].reshape(STRIP, H), at * RUN, RUN))
            right = wide[j, e].reshape(WIDE, H)
            part = -dot3(left, split(right), True)
            if e == 0:
                put_row_parts(part, j, mine, other, parts)
                wide_out[j] = right * t["o_deep"][j].astype(F32)
            else:
                base_out[j] = part


def far_part_kernel(parent, own, u1, u2, u3, d1, d2, d3, uh, dh, base, wide, mine, other, tall, parts):
    t = tree_of(parent)
    at = lax.axis_index("z")
    for step, piece in ((0, own), (1, u1), (2, u2), (3, u3), (-1, d1), (-2, d2), (-3, d3)):
        source = lax.rem(at + ZS - step, ZS)
        for k in range(NQ):
            tall[k, :, source] = piece[k].reshape(RS, FINE, H)
    source = lax.rem(at + ZS // 2, ZS)
    tall[0, :, source] = uh[0].reshape(RS, FINE, H)
    tall[1, :, source] = dh[0].reshape(RS, FINE, H)
    for j in range(NO):
        left = split(tall[t["o_slot"][j]].reshape(STRIP, H))
        part = base[j] - dot3(left, split(wide[j]), True)
        put_row_parts(part, j, mine, other, parts)


def near_solve_kernel(parent, *refs):
    pieces, q_pieces = refs[: 2 * YS], refs[2 * YS : 4 * YS]
    diag, fine, q_done, mean_out, square_out, load, held, own, rows, thin, sems, own_sems = refs[4 * YS :]
    t = tree_of(parent)
    x_at, z_at = lax.axis_index("x"), lax.axis_index("z")
    own_copies, copies = [], []
    for s in range(N):
        own_copies.append(pltpu.make_async_copy(fine.at[s, :, x_at, z_at], own.at[s], own_sems.at[s]))
        own_copies[-1].start()
    for j in range(NO):
        copies.append(pltpu.make_async_copy(diag.at[t["o"][j]], held.at[j], sems.at[j]))
        copies[-1].start()
    y_at, core_at = lax.axis_index("y"), lax.axis_index("core")
    for z in range(ZS):
        for step in range(YS):
            y = lax.rem(y_at + YS - step, YS)
            for side, source in ((core_at, q_pieces[step]), (1 - core_at, q_pieces[YS + step])):
                at = pl.multiple_of((y * CS + side) * FINE, FINE)
                thin[pl.ds(at, FINE)] = source[z, NQ][:, :128]
        flat = thin[...].T
        for x in range(XS):
            for s in range(N):
                to = 16 * x + 2 * z
                load[s, to : to + 2] = flat[16 * x + 2 * s : 16 * x + 2 * s + 2]
    for s in range(N):
        own_copies[s].wait()
        block = masked_rows(own[s].reshape(CHUNK, H), x_at * RUN + z_at * FINE, FINE)
        mean_out[s] = dot3(split(load[s]), split(block))
        square_out[s] = jnp.sum(block * block, axis=0, keepdims=True)
    for k in range(NQ):
        node = t["q"][k]
        done = q_done[k]
        mean_out[node] += dot3(split(load[t["q_par"][k]]), split(done))
        square_out[node] += jnp.sum(done * done, axis=0, keepdims=True)
    for j in range(NO):
        node = t["o"][j]
        rows_from(pieces, j, rows)
        copies[j].wait()
        done = dot3(split(rows[...]), split(masked_rows(held[j])))
        mean_out[node] += dot3(split(load[t["o_par"][j]]), split(done))
        square_out[node] += jnp.sum(done * done, axis=0, keepdims=True)


def far_solve_kernel(parent, *refs):
    pieces = refs[: 2 * YS]
    diag, mean_in, square_in, load, *out, held, mean, square, rows, sems = refs[2 * YS :]
    t = tree_of(parent)
    copies = []
    for j in range(NO):
        copies.append(pltpu.make_async_copy(diag.at[t["o"][j]], held.at[j], sems.at[j]))
        copies[-1].start()
    mean[...] = mean_in[...]
    square[...] = square_in[...]
    for j in range(NO):
        node = t["o"][j]
        rows_from(pieces, j, rows)
        copies[j].wait()
        done = dot3(split(rows[...]), split(masked_rows(held[j])))
        mean[node] += dot3(split(load[t["o_grand"][j]]), split(done))
        square[node] += jnp.sum(done * done, axis=0, keepdims=True)
    each = RHS // XS
    x_at = lax.axis_index("x")
    for step in range(XS):
        first = pl.multiple_of(lax.rem(x_at + step, XS) * each, each)
        for s in range(N):
            out[step][s] = mean[s, pl.ds(first, each)]
            out[step][N, s : s + 1] = square[s]
        out[step][N, N:] = jnp.zeros((each - N, H), F32)


def turn_kernel(a, b, c, d, *outs):
    outs, total, cut = outs[:ZS], outs[ZS], outs[ZS + 1]
    total[...] = (a[...] + b[...]) + (c[...] + d[...])
    each = RHS // (XS * ZS)
    for z in range(ZS):
        cut[z, 2 * N : 3 * N] = total[N, :N]
        cut[z, 3 * N :] = jnp.zeros((24 - 3 * N, H), F32)
        for s in range(N):
            cut[z, each * s : each * (s + 1)] = total[s, each * z : each * (z + 1)]
    at = lax.axis_index("z")
    for step in range(ZS):
        outs[step][...] = cut[lax.rem(at + step, ZS)]


def total_kernel(*refs):
    out = refs[ZS]
    total = refs[0][...]
    for step in range(1, ZS):
        total = total + refs[step][...]
    out[...] = total


def pair_kernel(mine, theirs, *outs):
    at = lax.axis_index("y")
    for step in range(YS):
        y = lax.rem(at + step, YS)
        outs[step][...] = mine[y] + theirs[y]


def sum_kernel(a, b, c, d, *refs):
    extra, outs, total = refs[: -ZS - 1], refs[-ZS - 1 : -1], refs[-1]
    total[...] = (a[...] + b[...]) + (c[...] + d[...])
    at = lax.axis_index("z")
    n = total.shape[1]
    for step in range(ZS):
        z = lax.rem(at + step, ZS)
        outs[step][:n] = total[z]
        for ref in extra:
            outs[step][n] = jnp.concatenate([ref[z], jnp.zeros((FINE, WIDE - 128), F32)], axis=1)


def stack_kernel(*refs):
    out = refs[ZS]
    at = lax.axis_index("z")
    for step in range(ZS):
        out[lax.rem(at + ZS - step, ZS)] = refs[step][...]


def shifted(array, axis, step):
    size = lax.axis_size(axis)
    return lax.ppermute(array, axis, [(i, (i + step) % size) for i in range(size)])


def by_distance(array, axis):
    return [array] + [shifted(array, axis, step) for step in range(1, lax.axis_size(axis))]


def across(outs, axis):
    return [outs[0]] + [shifted(part, axis, step) for step, part in enumerate(outs) if step]


def row_gathered(array):
    near = by_distance(array, "y")
    return near + [shifted(piece, "core", 1) for piece in near]


def summed_rows(mine, other, extra=()):
    n = mine.shape[2]
    paired = call(
        pair_kernel, tuple(shape(ZS, n, FINE, WIDE) for _ in range(YS)), [VMEM] * 2, [], 6
    )(mine, shifted(other, "core", 1))
    m = n + len(extra)
    return call(
        sum_kernel,
        tuple(shape(m, FINE, WIDE) for _ in range(ZS)),
        [VMEM] * (YS + len(extra)),
        [pltpu.VMEM((ZS, n, FINE, WIDE), F32)],
        6,
    )(*across(paired, "y"), *extra)


def stacked(pieces):
    return call(stack_kernel, shape(ZS, *pieces[0].shape), [VMEM] * ZS, [], 4)(*pieces)


def body(factor, diag, structure, parent, post):
    dma = pltpu.SemaphoreType.DMA
    blocks = jnp.transpose(factor, (0, 2, 3, 1))
    marks = jnp.transpose(structure, (0, 2, 1))
    thin = jnp.transpose(post, (0, 2, 1)).reshape(2 * N, H)
    runs = diag.reshape(N, RS, XS, RUN, H)
    fine = diag.reshape(N, RS, XS, ZS, FINE, H)
    q_pack, o_pack = call(
        pack_kernel,
        (shape(NQ * NARROW + 16, H), shape(NO, 2, NARROW, H)),
        [SMEM, SMEM, HBM, VMEM],
        [pltpu.VMEM((NQ + 2 * NO, NARROW, H), F32), dma((NQ + 2 * NO,))],
        6,
    )(parent, marks, blocks, thin)
    q_pieces = by_distance(q_pack, "x")
    o_pieces = by_distance(o_pack, "x")

    def parts_of(n):
        return (shape(YS, ZS, n, FINE, WIDE), shape(YS, ZS, n, FINE, WIDE))

    parts = pltpu.VMEM((YS, CS, ZS, FINE, WIDE), F32)
    q_mine, q_other, q_rhs = call(
        q_part_kernel,
        (*parts_of(NQ), shape(ZS, FINE, 128)),
        [SMEM, VMEM, VMEM, VMEM, VMEM, HBM],
        [
            pltpu.VMEM((NQ, RS, RUN, H), F32),
            pltpu.VMEM((NQ, XS, NARROW, H), F32),
            parts,
            pltpu.VMEM((128, H), F32),
            pltpu.VMEM((H, 128), F32),
            dma((NQ,)),
        ],
        16,
    )(parent, *q_pieces, runs)
    q_turned = across(summed_rows(q_mine, q_other, (q_rhs,)), "z")
    q_turned, o_pieces = lax.optimization_barrier((q_turned, o_pieces))
    q_all = row_gathered(stacked(q_turned))

    near_mine, near_other, base, o_wide = call(
        near_part_kernel,
        (*parts_of(NO), shape(NO, STRIP, WIDE), shape(NO, WIDE, H)),
        [SMEM, VMEM, VMEM, VMEM, VMEM, HBM],
        [pltpu.VMEM((NO, 2, RS, RUN, H), F32), pltpu.VMEM((NO, 2, XS, NARROW, H), F32), parts, dma((NO, 2))],
        30,
    )(parent, *o_pieces, runs)
    q_all, near_mine, near_other, base, o_wide = lax.optimization_barrier(
        (q_all, near_mine, near_other, base, o_wide)
    )
    q_done = call(
        q_solve_kernel,
        shape(NQ, CHUNK, H),
        [SMEM] + [VMEM] * (2 * YS) + [HBM],
        [pltpu.VMEM((NQ, W, H), F32), pltpu.VMEM((CHUNK, W), F32), dma((NQ,))],
        24,
    )(parent, *q_all, diag)
    near_mine, near_other, q_done = lax.optimization_barrier((near_mine, near_other, q_done))

    up, down = [q_done], [q_done]
    for _ in range(ZS // 2 - 1):
        up.append(shifted(up[-1], "z", 1))
        down.append(shifted(down[-1], "z", ZS - 1))
    up_half = shifted(up[-1][:1], "z", 1)
    down_half = shifted(down[-1][1:], "z", ZS - 1)
    near_own = summed_rows(near_mine, near_other)
    far_mine, far_other = call(
        far_part_kernel,
        parts_of(NO),
        [SMEM] + [VMEM] * 11,
        [pltpu.VMEM((NQ, RS, ZS, FINE, H), F32), parts],
        20,
    )(parent, *up, *down[1:], up_half, down_half, base, o_wide)
    near_turned = across(near_own, "z")
    far_own = summed_rows(far_mine, far_other)
    near_turned, far_own = lax.optimization_barrier((near_turned, far_own))
    near_all = row_gathered(stacked(near_turned))
    far_all = row_gathered(stacked(across(far_own, "z")))

    mean, square, load = call(
        near_solve_kernel,
        (shape(N, RHS, H), shape(N, 1, H), shape(N, RHS, CHUNK)),
        [SMEM] + [VMEM] * (4 * YS) + [HBM, HBM, VMEM],
        [
            pltpu.VMEM((NO, W, H), F32),
            pltpu.VMEM((N, RS, FINE, H), F32),
            pltpu.VMEM((CHUNK, W), F32),
            pltpu.VMEM((CHUNK, 128), F32),
            dma((NO,)),
            dma((N,)),
        ],
        30,
    )(parent, *near_all, *q_all, diag, fine, q_done)
    packed = call(
        far_solve_kernel,
        tuple(shape(N + 1, RHS // XS, H) for _ in range(XS)),
        [SMEM] + [VMEM] * (2 * YS) + [HBM] + [VMEM] * 3,
        [
            pltpu.VMEM((NO, W, H), F32),
            pltpu.VMEM((N, RHS, H), F32),
            pltpu.VMEM((N, 1, H), F32),
            pltpu.VMEM((CHUNK, W), F32),
            dma((NO,)),
        ],
        28,
    )(parent, *far_all, diag, mean, square, load)
    packed = call(
        turn_kernel,
        tuple(shape(24, H) for _ in range(ZS)),
        [VMEM] * XS,
        [pltpu.VMEM((N + 1, RHS // XS, H), F32), pltpu.VMEM((ZS, 24, H), F32)],
        4,
    )(*across(packed, "x"))
    total = call(total_kernel, shape(24, H), [VMEM] * ZS, [], 2)(*across(packed, "z"))
    mean_x = jnp.transpose(total[: 2 * N].reshape(N, 2, H), (0, 2, 1))
    return mean_x, total[2 * N : 3 * N]


def solution(mesh):
    finer = Mesh(mesh.devices.reshape(YS, CS, ZS, XS), (*ROW, *COL))
    placed = (
        P(None, ROW, None, COL),
        P(None, None, ROW),
        P(None, None, ROW),
        P(),
        P(None, ROW, COL),
    )
    return jax.shard_map(
        body,
        mesh=finer,
        in_specs=placed,
        out_specs=(P(None, ROW, COL), P(None, ROW)),
        check_vma=False,
    )
```

```python
import jax
import jax.numpy as jnp
from jax import lax
from jax.experimental import pallas as pl
from jax.experimental.pallas import tpu as pltpu
from jax.sharding import Mesh
from jax.sharding import PartitionSpec as P

ROW = ("y", "core")
COL = ("z", "x")
F32 = jnp.float32
BF16 = jnp.bfloat16

N = 6
W = 2048
H = 256
YS, CS, ZS, XS = 4, 2, 8, 4
RS = YS * CS
NARROW = W // (ZS * XS)
WIDE = NARROW * XS
STRIP = W // XS
CHUNK = STRIP // ZS
FINE = CHUNK // RS
RUN = STRIP // RS
HALF = W // ZS
SLAB = NARROW * ZS
NQ, NO = 2, 4
RHS = 64

SMEM = pl.BlockSpec(memory_space=pltpu.SMEM)
VMEM = pl.BlockSpec(memory_space=pltpu.VMEM)
HBM = pl.BlockSpec(memory_space=pltpu.HBM)


def call(kernel, outs, in_specs, scratch, mib, flops=10**9):
    return pl.pallas_call(
        kernel,
        out_shape=outs,
        cost_estimate=pl.CostEstimate(flops=flops, bytes_accessed=10**7, transcendentals=0),
        in_specs=in_specs,
        out_specs=jax.tree.map(lambda _: VMEM, outs),
        scratch_shapes=scratch,
        compiler_params=pltpu.CompilerParams(vmem_limit_bytes=mib * 1024 * 1024),
    )


def named(*args):
    def run(*operands):
        return call(*args)(*operands)

    return run


def shape(*dims):
    return jax.ShapeDtypeStruct(dims, F32)


def tree_of(parent_ref):
    par = [parent_ref[i] for i in range(N)]
    zero = jnp.int32(0)
    q, q_ok, o, o_ok = [zero] * NQ, [zero] * NQ, [zero] * NO, [zero] * NO
    q_count = o_count = zero
    for i in range(N):
        has_parent = (par[i] < N).astype(jnp.int32)
        has_child = zero
        for s in range(i):
            has_child = has_child | (par[s] == i).astype(jnp.int32)
        inner = has_parent * has_child
        outer = has_parent * (1 - has_child)
        for k in range(NQ):
            hit = inner * (q_count == k).astype(jnp.int32)
            q[k] = jnp.where(hit == 1, i, q[k])
            q_ok[k] = q_ok[k] | hit
        for k in range(NO):
            hit = outer * (o_count == k).astype(jnp.int32)
            o[k] = jnp.where(hit == 1, i, o[k])
            o_ok[k] = o_ok[k] | hit
        q_count = q_count + inner
        o_count = o_count + outer
    last = N - 1
    q_par = [jnp.minimum(parent_ref[v], last) for v in q]
    o_up = [parent_ref[v] for v in o]
    o_par = [jnp.minimum(v, last) for v in o_up]
    o_over = [jnp.where(up < N, parent_ref[v], N) for up, v in zip(o_up, o_par)]
    o_grand = [jnp.minimum(v, last) for v in o_over]
    o_deep = [ok * (v < N).astype(jnp.int32) for ok, v in zip(o_ok, o_over)]
    o_slot = [q_ok[1] * (v == q[1]).astype(jnp.int32) for v in o_par]
    return dict(
        q=q, q_ok=q_ok, q_par=q_par, o=o, o_ok=o_ok, o_par=o_par, o_grand=o_grand, o_deep=o_deep, o_slot=o_slot
    )


def split(a):
    high = a.astype(BF16)
    return high, (a - high.astype(F32)).astype(BF16)


def dot3(a, b, transposed=False):
    dims = (((1,), (1 if transposed else 0,)), ((), ()))
    mul = lambda u, v: lax.dot_general(u, v, dims, preferred_element_type=F32)
    ah, al = a
    bh, bl = b
    return mul(ah, bh) + (mul(ah, bl) + mul(al, bh))


def masked_rows(block, row_of):
    rows = row_of(lax.broadcasted_iota(jnp.int32, block.shape, 0))
    cols = lax.axis_index(ROW) * H + lax.broadcasted_iota(jnp.int32, block.shape, 1)
    return jnp.where(rows >= cols, block, 0.0)


def put_row_parts(part, index, mine, other, parts):
    core = lax.axis_index("core")
    parts[...] = part.reshape(parts.shape)
    mine[:, :, index] = parts[:, core]
    other[:, :, index] = parts[:, 1 - core]


def pack_kernel(parent, marks, factor, thin, q_out, o_out, held, sems):
    t = tree_of(parent)
    slots = [(t["q_par"][k], t["q"][k], t["q_ok"][k]) for k in range(NQ)]
    for j in range(NO):
        slots.append((t["o_par"][j], t["o"][j], t["o_ok"][j]))
        slots.append((t["o_grand"][j], t["o"][j], t["o_deep"][j]))
    copies = []
    for n, (up, node, _) in enumerate(slots):
        copies.append(pltpu.make_async_copy(factor.at[up, node], held.at[n], sems.at[n]))
        copies[-1].start()
    left = lax.broadcasted_iota(jnp.int32, (NARROW, H), 1) < H // 2
    q_out[NQ * NARROW : NQ * NARROW + 2 * N] = thin[...]
    q_out[NQ * NARROW + 2 * N :] = jnp.zeros((16 - 2 * N, H), F32)
    for n, (up, node, ok) in enumerate(slots):
        copies[n].wait()
        first = (marks[node, 0, up] * ok).astype(F32)
        second = (marks[node, 1, up] * ok).astype(F32)
        block = held[n] * jnp.where(left, first, second)
        if n < NQ:
            q_out[n * NARROW : (n + 1) * NARROW] = block
        else:
            o_out[(n - NQ) // 2, (n - NQ) % 2] = block


def q_part_kernel(parent, p0, p1, p2, p3, diag, mine, other, rhs_out, strip, wide, parts, thin, tall, sems):
    t = tree_of(parent)
    at = lax.axis_index("x")
    copies = []
    for k in range(NQ):
        copies.append(pltpu.make_async_copy(diag.at[t["q_par"][k], :, at], strip.at[k], sems.at[k]))
        copies[-1].start()
    row_of = lambda i: (i // RUN) * H + at * RUN + i % RUN
    thin[...] = jnp.zeros_like(thin)
    for step, piece in enumerate((p0, p1, p2, p3)):
        source = lax.rem(at + XS - step, XS)
        for k in range(NQ):
            wide[k, source] = piece[k * NARROW : (k + 1) * NARROW]
        thin[pl.ds(pl.multiple_of(source * 16, 16), 16)] = piece[NQ * NARROW :]
    tall[...] = thin[...].T
    rhs_out[...] = tall[pl.ds(pl.multiple_of(at * RUN, RUN), RUN)].reshape(ZS, FINE, 128)
    for k in range(NQ):
        copies[k].wait()
        left = split(masked_rows(strip[k].reshape(STRIP, H), row_of))
        part = -dot3(left, split(wide[k].reshape(WIDE, H)), True)
        put_row_parts(part, k, mine, other, parts)


def rows_from(pieces, slot, rows):
    y_at, core_at = lax.axis_index("y"), lax.axis_index("core")
    for step in range(YS):
        y = lax.rem(y_at + YS - step, YS)
        for side, source in ((core_at, pieces[step]), (1 - core_at, pieces[YS + step])):
            first = pl.multiple_of((y * CS + side) * FINE, FINE)
            width = source.shape[-1]
            for b in range(source.shape[0]):
                rows[pl.ds(first, FINE), b * width : (b + 1) * width] = source[b, slot]


def q_solve_kernel(parent, *refs):
    pieces, (diag, out, rows, held, sems) = refs[: 2 * YS], refs[2 * YS :]
    t = tree_of(parent)
    copies = []
    for k in range(NQ):
        copies.append(pltpu.make_async_copy(diag.at[t["q"][k]], held.at[k], sems.at[k]))
        copies[-1].start()
    for k in range(NQ):
        rows_from(pieces, k, rows)
        copies[k].wait()
        block = held[k].reshape(W, H)
        out[k] = dot3(split(rows[...]), split(masked_rows(block, lambda i: i)))


def outer_solve(pieces, j, node, diag, rows):
    rows_from(pieces, j, rows)
    done = None
    for x in range(XS):
        block = masked_rows(
            diag[node, :, x].reshape(SLAB, H), lambda i: (i // NARROW) * WIDE + x * NARROW + i % NARROW
        )
        part = dot3(split(rows[:, x * SLAB : (x + 1) * SLAB]), split(block))
        done = part if done is None else done + part
    return done


def near_part_kernel(parent, *refs):
    own, u1, u2, u3, d1, d2, d3, uh, dh = refs[:9]
    diag, mine, other, base_out, wide_out, wide, parts, strip, sems = refs[9:]
    t = tree_of(parent)
    at = lax.axis_index("z")
    copies = []
    for j in range(NO):
        for e, node in enumerate((t["o_par"][j], t["o_grand"][j])):
            copies.append(pltpu.make_async_copy(diag.at[node, :, :, at], strip.at[j, e], sems.at[j, e]))
            copies[-1].start()
    for step, piece in ((0, own), (1, u1), (2, u2), (3, u3), (-1, d1), (-2, d2), (-3, d3)):
        source = lax.rem(at + ZS - step, ZS)
        for j in range(NO):
            for e in range(2):
                wide[j, e, source] = piece[j, e]
    source = lax.rem(at + ZS // 2, ZS)
    for j in range(NO // 2):
        for e in range(2):
            wide[j, e, source] = uh[j, e]
            wide[NO // 2 + j, e, source] = dh[j, e]
    row_of = lambda i: (i // (XS * FINE)) * H + (i // FINE) % XS * RUN + at * FINE + i % FINE
    for j in range(NO):
        for e in range(2):
            copies[2 * j + e].wait()
            left = split(masked_rows(strip[j, e].reshape(HALF, H), row_of))
            right = wide[j, e].reshape(SLAB, H)
            part = -dot3(left, split(right), True)
            if e == 0:
                put_row_parts(part, j, mine, other, parts)
                wide_out[j] = right * t["o_deep"][j].astype(F32)
            else:
                base_out[j] = part


def far_part_kernel(parent, a, b, c, d, base, wide, mine, other, tall, parts):
    t = tree_of(parent)
    at = lax.axis_index("x")
    for step, piece in enumerate((a, b, c, d)):
        source = lax.rem(at + XS - step, XS)
        for k in range(NQ):
            tall[k, :, source] = piece[k].reshape(RS, FINE, H)
    for j in range(NO):
        left = split(tall[t["o_slot"][j]].reshape(HALF, H))
        part = base[j] - dot3(left, split(wide[j]), True)
        put_row_parts(part, j, mine, other, parts)


def near_solve_kernel(parent, *refs):
    pieces, q_pieces = refs[: 2 * YS], refs[2 * YS : 4 * YS]
    diag, q_done, mean_out, square_out, load, rows, thin = refs[4 * YS :]
    t = tree_of(parent)
    x_at, z_at = lax.axis_index("x"), lax.axis_index("z")
    y_at, core_at = lax.axis_index("y"), lax.axis_index("core")
    for z in range(ZS):
        for step in range(YS):
            y = lax.rem(y_at + YS - step, YS)
            for side, source in ((core_at, q_pieces[step]), (1 - core_at, q_pieces[YS + step])):
                at = pl.multiple_of((y * CS + side) * FINE, FINE)
                thin[pl.ds(at, FINE)] = source[z, NQ][:, :128]
        flat = thin[...].T
        for x in range(XS):
            for s in range(N):
                to = 16 * x + 2 * z
                load[s, to : to + 2] = flat[16 * x + 2 * s : 16 * x + 2 * s + 2]
    for s in range(N):
        block = masked_rows(
            diag[s, :, x_at, z_at].reshape(CHUNK, H), lambda i: (i // FINE) * H + x_at * RUN + z_at * FINE + i % FINE
        )
        mean_out[s] = dot3(split(load[s]), split(block))
        square_out[s] = jnp.sum(block * block, axis=0, keepdims=True)
    for k in range(NQ):
        node = t["q"][k]
        done = q_done[k]
        mean_out[node] += dot3(split(load[t["q_par"][k]]), split(done))
        square_out[node] += jnp.sum(done * done, axis=0, keepdims=True)
    for j in range(NO):
        node = t["o"][j]
        done = outer_solve(pieces, j, node, diag, rows)
        mean_out[node] += dot3(split(load[t["o_par"][j]]), split(done))
        square_out[node] += jnp.sum(done * done, axis=0, keepdims=True)


def far_solve_kernel(parent, *refs):
    pieces = refs[: 2 * YS]
    diag, mean_in, square_in, load, *out, mean, square, rows = refs[2 * YS :]
    t = tree_of(parent)
    mean[...] = mean_in[...]
    square[...] = square_in[...]
    for j in range(NO):
        node = t["o"][j]
        done = outer_solve(pieces, j, node, diag, rows)
        mean[node] += dot3(split(load[t["o_grand"][j]]), split(done))
        square[node] += jnp.sum(done * done, axis=0, keepdims=True)
    each = RHS // XS
    x_at = lax.axis_index("x")
    for step in range(XS):
        first = pl.multiple_of(lax.rem(x_at + step, XS) * each, each)
        for s in range(N):
            out[step][s] = mean[s, pl.ds(first, each)]
            out[step][N, s : s + 1] = square[s]
        out[step][N, N:] = jnp.zeros((each - N, H), F32)


def turn_kernel(a, b, c, d, cut, total):
    total[...] = (a[...] + b[...]) + (c[...] + d[...])
    each = RHS // (XS * ZS)
    for z in range(ZS):
        cut[z, 2 * N : 3 * N] = total[N, :N]
        cut[z, 3 * N :] = jnp.zeros((24 - 3 * N, H), F32)
        for s in range(N):
            cut[z, each * s : each * (s + 1)] = total[s, each * z : each * (z + 1)]


def total_kernel(parts, out):
    total = parts[0]
    for step in range(1, ZS):
        total = total + parts[step]
    out[...] = total


def pair_kernel(mine, theirs, *outs):
    at = lax.axis_index("y")
    for step in range(YS):
        y = lax.rem(at + step, YS)
        outs[step][...] = mine[y] + theirs[y]


def q_sum_kernel(a, b, c, d, extra, out):
    for z in range(ZS):
        out[z, :NQ] = (a[z] + b[z]) + (c[z] + d[z])
        out[z, NQ] = jnp.concatenate([extra[z], jnp.zeros((FINE, WIDE - 128), F32)], axis=1)


def sum_kernel(a, b, c, d, *outs):
    at = lax.axis_index("x")
    for step in range(XS):
        x = lax.rem(at + step, XS)
        outs[step][...] = (a[x] + b[x]) + (c[x] + d[x])


def stack_kernel(*refs):
    out = refs[XS]
    at = lax.axis_index("x")
    for step in range(XS):
        out[lax.rem(at + XS - step, XS)] = refs[step][...]


def shifted(array, axis, step):
    size = lax.axis_size(axis)
    return lax.ppermute(array, axis, [(i, (i + step) % size) for i in range(size)])


def by_distance(array, axis):
    return [array] + [shifted(array, axis, step) for step in range(1, lax.axis_size(axis))]


def across(outs, axis):
    return [outs[0]] + [shifted(part, axis, step) for step, part in enumerate(outs) if step]


def row_gathered(array):
    near = by_distance(array, "y")
    return near + [shifted(piece, "core", 1) for piece in near]


def ringed(array, axis):
    size = lax.axis_size(axis)
    up, down = [array], [array]
    for _ in range(size // 2 - 1):
        up.append(shifted(up[-1], axis, 1))
        down.append(shifted(down[-1], axis, size - 1))
    half = array.shape[0] // 2
    return up + down[1:] + [shifted(up[-1][:half], axis, 1), shifted(down[-1][half:], axis, size - 1)]


def paired_rows(mine, other):
    outs = tuple(shape(*mine.shape[1:]) for _ in range(YS))
    return across(call(pair_kernel, outs, [VMEM] * 2, [], 6)(mine, shifted(other, "core", 1)), "y")


def summed_rows(mine, other):
    outs = tuple(shape(*mine.shape[2:]) for _ in range(XS))
    return call(sum_kernel, outs, [VMEM] * YS, [], 6)(*paired_rows(mine, other))


def stacked(pieces):
    return call(stack_kernel, shape(XS, *pieces[0].shape), [VMEM] * XS, [], 4)(*pieces)


def program(factor, diag, structure, parent, post):
    dma = pltpu.SemaphoreType.DMA
    blocks = jnp.transpose(factor, (0, 2, 3, 1))
    marks = jnp.transpose(structure, (0, 2, 1))
    thin = jnp.transpose(post, (0, 2, 1)).reshape(2 * N, H)
    fine = diag.reshape(N, RS, XS, ZS, FINE, H)
    q_pack, o_pack = call(
        pack_kernel,
        (shape(NQ * NARROW + 16, H), shape(NO, 2, NARROW, H)),
        [SMEM, SMEM, HBM, VMEM],
        [pltpu.VMEM((NQ + 2 * NO, NARROW, H), F32), dma((NQ + 2 * NO,))],
        6,
    )(parent, marks, blocks, thin)
    q_pieces = by_distance(q_pack, "x")
    o_pieces = ringed(o_pack, "z")

    def parts_of(*dims):
        return (shape(YS, *dims), shape(YS, *dims))

    q_mine, q_other, q_rhs = call(
        q_part_kernel,
        (*parts_of(ZS, NQ, FINE, WIDE), shape(ZS, FINE, 128)),
        [SMEM, VMEM, VMEM, VMEM, VMEM, HBM],
        [
            pltpu.VMEM((NQ, RS, ZS, FINE, H), F32),
            pltpu.VMEM((NQ, XS, NARROW, H), F32),
            pltpu.VMEM((YS, CS, ZS, FINE, WIDE), F32),
            pltpu.VMEM((128, H), F32),
            pltpu.VMEM((H, 128), F32),
            dma((NQ,)),
        ],
        50,
    )(parent, *q_pieces, fine)
    q_sum = call(q_sum_kernel, shape(ZS, NQ + 1, FINE, WIDE), [VMEM] * 5, [], 6)(*paired_rows(q_mine, q_other), q_rhs)
    q_all = row_gathered(lax.all_to_all(q_sum, "z", 0, 0, tiled=True))
    q_done = call(
        q_solve_kernel,
        shape(NQ, CHUNK, H),
        [SMEM] + [VMEM] * (2 * YS) + [HBM],
        [pltpu.VMEM((CHUNK, W), F32), pltpu.VMEM((NQ, RS, XS, ZS, FINE, H), F32), dma((NQ,))],
        50,
    )(parent, *q_all, fine)

    done_pieces = by_distance(q_done, "x")
    parts = pltpu.VMEM((YS, CS, XS, FINE, SLAB), F32)
    near_mine, near_other, base, o_wide = named(
        near_part_kernel,
        (*parts_of(XS, NO, FINE, SLAB), shape(NO, HALF, SLAB), shape(NO, SLAB, H)),
        [SMEM] + [VMEM] * 9 + [HBM],
        [
            pltpu.VMEM((NO, 2, ZS, NARROW, H), F32),
            parts,
            pltpu.VMEM((NO, 2, RS, XS, FINE, H), F32),
            dma((NO, 2)),
        ],
        44,
    )(parent, *o_pieces, fine)
    near_sum = summed_rows(near_mine, near_other)
    far_mine, far_other = call(
        far_part_kernel,
        parts_of(XS, NO, FINE, SLAB),
        [SMEM] + [VMEM] * 6,
        [pltpu.VMEM((NQ, RS, XS, FINE, H), F32), parts],
        20,
    )(parent, *done_pieces, base, o_wide)
    far_sum = summed_rows(far_mine, far_other)
    near_all = row_gathered(stacked(across(near_sum, "x")))
    far_near = by_distance(stacked(across(far_sum, "x")), "y")

    mean, square, load = call(
        near_solve_kernel,
        (shape(N, RHS, H), shape(N, 1, H), shape(N, RHS, CHUNK)),
        [SMEM] + [VMEM] * (4 * YS) + [VMEM, VMEM],
        [pltpu.VMEM((CHUNK, W), F32), pltpu.VMEM((CHUNK, 128), F32)],
        30,
    )(parent, *near_all, *q_all, fine, q_done)
    mean, square, load, *far_near = lax.optimization_barrier((mean, square, load, *far_near))
    far_all = far_near + [shifted(piece, "core", 1) for piece in far_near]
    packed = call(
        far_solve_kernel,
        tuple(shape(N + 1, RHS // XS, H) for _ in range(XS)),
        [SMEM] + [VMEM] * (2 * YS) + [VMEM] * 4,
        [pltpu.VMEM((N, RHS, H), F32), pltpu.VMEM((N, 1, H), F32), pltpu.VMEM((CHUNK, W), F32)],
        30,
    )(parent, *far_all, fine, mean, square, load)
    packed = call(
        turn_kernel, shape(ZS, 24, H), [VMEM] * XS, [pltpu.VMEM((N + 1, RHS // XS, H), F32)], 4
    )(*across(packed, "x"))
    total = call(total_kernel, shape(24, H), [VMEM], [], 4)(lax.all_to_all(packed, "z", 0, 0, tiled=True))
    mean_x = jnp.transpose(total[: 2 * N].reshape(N, 2, H), (0, 2, 1))
    return mean_x, total[2 * N : 3 * N]


def solution(mesh):
    finer = Mesh(mesh.devices.reshape(YS, CS, ZS, XS), (*ROW, *COL))
    placed = (
        P(None, ROW, None, COL),
        P(None, None, ROW),
        P(None, None, ROW),
        P(),
        P(None, ROW, COL),
    )
    return jax.shard_map(
        program,
        mesh=finer,
        in_specs=placed,
        out_specs=(P(None, ROW, COL), P(None, ROW)),
        check_vma=False,
    )
```

```python
import functools

import jax
import jax.numpy as jnp
from jax import lax
from jax.experimental import pallas as pl
from jax.experimental.pallas import tpu as pltpu
from jax.sharding import Mesh
from jax.sharding import PartitionSpec as P

ROW = ("y", "core")
COL = ("z", "x")
F32 = jnp.float32
BF16 = jnp.bfloat16

N = 6
W = 2048
H = 256
YS, CS, ZS, XS = 4, 2, 8, 4
RS = YS * CS
NARROW = W // (ZS * XS)
WIDE = NARROW * XS
STRIP = W // XS
CHUNK = STRIP // ZS
FINE = CHUNK // RS
RUN = STRIP // RS
HALF = W // ZS
SLAB = NARROW * ZS
NQ, NO = 2, 4
RHS = 64

SMEM = pl.BlockSpec(memory_space=pltpu.SMEM)
VMEM = pl.BlockSpec(memory_space=pltpu.VMEM)
HBM = pl.BlockSpec(memory_space=pltpu.HBM)


def call(kernel, outs, in_specs, scratch, mib, flops=10**9):
    return pl.pallas_call(
        kernel,
        out_shape=outs,
        cost_estimate=pl.CostEstimate(flops=flops, bytes_accessed=10**7, transcendentals=0),
        in_specs=in_specs,
        out_specs=jax.tree.map(lambda _: VMEM, outs),
        scratch_shapes=scratch,
        compiler_params=pltpu.CompilerParams(vmem_limit_bytes=mib * 1024 * 1024),
    )


def named(*args):
    def run(*operands):
        return call(*args)(*operands)

    return run


def shape(*dims):
    return jax.ShapeDtypeStruct(dims, F32)


def tree_of(parent_ref):
    par = [parent_ref[i] for i in range(N)]
    zero = jnp.int32(0)
    q, q_ok, o, o_ok = [zero] * NQ, [zero] * NQ, [zero] * NO, [zero] * NO
    q_count = o_count = zero
    for i in range(N):
        has_parent = (par[i] < N).astype(jnp.int32)
        has_child = zero
        for s in range(i):
            has_child = has_child | (par[s] == i).astype(jnp.int32)
        inner = has_parent * has_child
        outer = has_parent * (1 - has_child)
        for k in range(NQ):
            hit = inner * (q_count == k).astype(jnp.int32)
            q[k] = jnp.where(hit == 1, i, q[k])
            q_ok[k] = q_ok[k] | hit
        for k in range(NO):
            hit = outer * (o_count == k).astype(jnp.int32)
            o[k] = jnp.where(hit == 1, i, o[k])
            o_ok[k] = o_ok[k] | hit
        q_count = q_count + inner
        o_count = o_count + outer
    last = N - 1
    q_par = [jnp.minimum(parent_ref[v], last) for v in q]
    o_up = [parent_ref[v] for v in o]
    o_par = [jnp.minimum(v, last) for v in o_up]
    o_over = [jnp.where(up < N, parent_ref[v], N) for up, v in zip(o_up, o_par)]
    o_grand = [jnp.minimum(v, last) for v in o_over]
    o_deep = [ok * (v < N).astype(jnp.int32) for ok, v in zip(o_ok, o_over)]
    o_slot = [q_ok[1] * (v == q[1]).astype(jnp.int32) for v in o_par]
    return dict(
        q=q, q_ok=q_ok, q_par=q_par, o=o, o_ok=o_ok, o_par=o_par, o_grand=o_grand, o_deep=o_deep, o_slot=o_slot
    )


def at_index(values, index):
    result = values[0]
    for n in range(1, len(values)):
        result = jnp.where(index == n, values[n], result)
    return result


def each(number, step):
    def run(index, carry):
        step(index)
        return carry

    lax.fori_loop(0, number, run, 0)


def split(a):
    high = a.astype(BF16)
    return high, (a - high.astype(F32)).astype(BF16)


def dot3(a, b, transposed=False):
    dims = (((1,), (1 if transposed else 0,)), ((), ()))
    mul = lambda u, v: lax.dot_general(u, v, dims, preferred_element_type=F32)
    ah, al = a
    bh, bl = b
    return mul(ah, bh) + (mul(ah, bl) + mul(al, bh))


def masked_rows(block, row_of):
    rows = row_of(lax.broadcasted_iota(jnp.int32, block.shape, 0))
    cols = lax.axis_index(ROW) * H + lax.broadcasted_iota(jnp.int32, block.shape, 1)
    return jnp.where(rows >= cols, block, 0.0)


def put_row_parts(part, index, mine, other, parts):
    core = lax.axis_index("core")
    parts[...] = part.reshape(parts.shape)
    mine[:, :, index] = parts[:, core]
    other[:, :, index] = parts[:, 1 - core]


def pack_kernel(parent, marks, factor, thin, q_out, o_out, held, sems):
    t = tree_of(parent)
    slots = [(t["q_par"][k], t["q"][k], t["q_ok"][k]) for k in range(NQ)]
    for j in range(NO):
        slots.append((t["o_par"][j], t["o"][j], t["o_ok"][j]))
        slots.append((t["o_grand"][j], t["o"][j], t["o_deep"][j]))
    copies = []
    for n, (up, node, _) in enumerate(slots):
        copies.append(pltpu.make_async_copy(factor.at[up, node], held.at[n], sems.at[n]))
        copies[-1].start()
    left = lax.broadcasted_iota(jnp.int32, (NARROW, H), 1) < H // 2
    for s in range(N):
        q_out[NQ * NARROW + 2 * s : NQ * NARROW + 2 * s + 2] = thin[s]
    q_out[NQ * NARROW + 2 * N :] = jnp.zeros((16 - 2 * N, H), F32)
    for n, (up, node, ok) in enumerate(slots):
        copies[n].wait()
        first = (marks[node, 0, up] * ok).astype(F32)
        second = (marks[node, 1, up] * ok).astype(F32)
        block = held[n] * jnp.where(left, first, second)
        if n < NQ:
            q_out[n * NARROW : (n + 1) * NARROW] = block
        else:
            o_out[(n - NQ) // 2, (n - NQ) % 2] = block


def q_part_kernel(parent, p0, p1, p2, p3, diag, mine, other, rhs_out, strip, wide, parts, thin, tall, sems):
    t = tree_of(parent)
    at = lax.axis_index("x")
    copies = []
    for k in range(NQ):
        copies.append(pltpu.make_async_copy(diag.at[t["q_par"][k], :, at], strip.at[k], sems.at[k]))
        copies[-1].start()
    row_of = lambda i: (i // RUN) * H + at * RUN + i % RUN
    thin[...] = jnp.zeros_like(thin)
    for step, piece in enumerate((p0, p1, p2, p3)):
        source = lax.rem(at + XS - step, XS)
        for k in range(NQ):
            wide[k, source] = piece[k * NARROW : (k + 1) * NARROW]
        thin[pl.ds(pl.multiple_of(source * 16, 16), 16)] = piece[NQ * NARROW :]
    tall[...] = thin[...].T
    rhs_out[...] = tall[pl.ds(pl.multiple_of(at * RUN, RUN), RUN)].reshape(ZS, FINE, 128)
    for k in range(NQ):
        copies[k].wait()
        left = split(masked_rows(strip[k].reshape(STRIP, H), row_of))
        part = -dot3(left, split(wide[k].reshape(WIDE, H)), True)
        put_row_parts(part, k, mine, other, parts)


def rows_from(pieces, slot, rows):
    y_at, core_at = lax.axis_index("y"), lax.axis_index("core")
    for step in range(YS):
        y = lax.rem(y_at + YS - step, YS)
        for side, source in ((core_at, pieces[step]), (1 - core_at, pieces[YS + step])):
            first = pl.multiple_of((y * CS + side) * FINE, FINE)
            width = source.shape[-1]
            for b in range(source.shape[0]):
                rows[pl.ds(first, FINE), b * width : (b + 1) * width] = source[b, slot]


def q_solve_kernel(parent, *refs):
    pieces, (diag, out, rows, held, sems) = refs[: 2 * YS], refs[2 * YS :]
    t = tree_of(parent)
    copies = []
    for k in range(NQ):
        copies.append(pltpu.make_async_copy(diag.at[t["q"][k]], held.at[k], sems.at[k]))
        copies[-1].start()
    for k in range(NQ):
        copies[k].wait()

    @functools.partial(each, NQ)
    def _(k):
        rows_from(pieces, k, rows)
        block = held[k].reshape(W, H)
        out[k] = dot3(split(rows[...]), split(masked_rows(block, lambda i: i)))


def outer_solve(pieces, j, node, diag, rows):
    rows_from(pieces, j, rows)
    done = None
    for x in range(XS):
        block = masked_rows(
            diag[node, :, x].reshape(SLAB, H), lambda i: (i // NARROW) * WIDE + x * NARROW + i % NARROW
        )
        part = dot3(split(rows[:, x * SLAB : (x + 1) * SLAB]), split(block))
        done = part if done is None else done + part
    return done


def near_part_kernel(parent, *refs):
    own, u1, u2, u3, d1, d2, d3, uh, dh = refs[:9]
    diag, mine, other, base_out, wide_out, wide, parts, strip, sems = refs[9:]
    t = tree_of(parent)
    at = lax.axis_index("z")
    copies = []
    for j in range(NO):
        for e, node in enumerate((t["o_par"][j], t["o_grand"][j])):
            copies.append(pltpu.make_async_copy(diag.at[node, :, :, at], strip.at[j, e], sems.at[j, e]))
            copies[-1].start()
    for step, piece in ((0, own), (1, u1), (2, u2), (3, u3), (-1, d1), (-2, d2), (-3, d3)):
        source = lax.rem(at + ZS - step, ZS)
        for j in range(NO):
            for e in range(2):
                wide[j, e, source] = piece[j, e]
    source = lax.rem(at + ZS // 2, ZS)
    for j in range(NO // 2):
        for e in range(2):
            wide[j, e, source] = uh[j, e]
            wide[NO // 2 + j, e, source] = dh[j, e]
    row_of = lambda i: (i // (XS * FINE)) * H + (i // FINE) % XS * RUN + at * FINE + i % FINE
    for j in range(NO):
        for e in range(2):
            copies[2 * j + e].wait()

    @functools.partial(each, NO)
    def _(j):
        for e in range(2):
            left = split(masked_rows(strip[j, e].reshape(HALF, H), row_of))
            right = wide[j, e].reshape(SLAB, H)
            part = -dot3(left, split(right), True)
            if e == 0:
                put_row_parts(part, j, mine, other, parts)
                wide_out[j] = right * at_index(t["o_deep"], j).astype(F32)
            else:
                base_out[j] = part


def far_part_kernel(parent, a, b, c, d, base, wide, mine, other, tall, parts):
    t = tree_of(parent)
    at = lax.axis_index("x")
    for step, piece in enumerate((a, b, c, d)):
        source = lax.rem(at + XS - step, XS)
        for k in range(NQ):
            tall[k, :, source] = piece[k].reshape(RS, FINE, H)

    @functools.partial(each, NO)
    def _(j):
        left = split(tall[at_index(t["o_slot"], j)].reshape(HALF, H))
        part = base[j] - dot3(left, split(wide[j]), True)
        put_row_parts(part, j, mine, other, parts)


def near_solve_kernel(parent, *refs):
    pieces, q_pieces = refs[: 2 * YS], refs[2 * YS : 4 * YS]
    diag, q_done, mean_out, square_out, load, rows, thin = refs[4 * YS :]
    t = tree_of(parent)
    x_at, z_at = lax.axis_index("x"), lax.axis_index("z")
    y_at, core_at = lax.axis_index("y"), lax.axis_index("core")
    for z in range(ZS):
        for step in range(YS):
            y = lax.rem(y_at + YS - step, YS)
            for side, source in ((core_at, q_pieces[step]), (1 - core_at, q_pieces[YS + step])):
                at = pl.multiple_of((y * CS + side) * FINE, FINE)
                thin[pl.ds(at, FINE)] = source[z, NQ][:, :128]
        flat = thin[...].T
        for x in range(XS):
            for s in range(N):
                to = 16 * x + 2 * z
                load[s, to : to + 2] = flat[16 * x + 2 * s : 16 * x + 2 * s + 2]
    for s in range(N):
        block = masked_rows(
            diag[s, :, x_at, z_at].reshape(CHUNK, H), lambda i: (i // FINE) * H + x_at * RUN + z_at * FINE + i % FINE
        )
        mean_out[s] = dot3(split(load[s]), split(block))
        square_out[s] = jnp.sum(block * block, axis=0, keepdims=True)
    for k in range(NQ):
        node = t["q"][k]
        done = q_done[k]
        mean_out[node] += dot3(split(load[t["q_par"][k]]), split(done))
        square_out[node] += jnp.sum(done * done, axis=0, keepdims=True)

    @functools.partial(each, NO)
    def _(j):
        node = at_index(t["o"], j)
        done = outer_solve(pieces, j, node, diag, rows)
        mean_out[node] += dot3(split(load[at_index(t["o_par"], j)]), split(done))
        square_out[node] += jnp.sum(done * done, axis=0, keepdims=True)


def far_solve_kernel(parent, *refs):
    pieces = refs[: 2 * YS]
    diag, mean_in, square_in, load, *out, mean, square, rows = refs[2 * YS :]
    t = tree_of(parent)
    mean[...] = mean_in[...]
    square[...] = square_in[...]

    @functools.partial(each, NO)
    def _(j):
        node = at_index(t["o"], j)
        done = outer_solve(pieces, j, node, diag, rows)
        mean[node] += dot3(split(load[at_index(t["o_grand"], j)]), split(done))
        square[node] += jnp.sum(done * done, axis=0, keepdims=True)

    share = RHS // XS
    x_at = lax.axis_index("x")
    for step in range(XS):
        first = pl.multiple_of(lax.rem(x_at + step, XS) * share, share)
        for s in range(N):
            out[step][s] = mean[s, pl.ds(first, share)]
            out[step][N, s : s + 1] = square[s]
        out[step][N, N:] = jnp.zeros((share - N, H), F32)


def turn_kernel(a, b, c, d, cut, total):
    total[...] = (a[...] + b[...]) + (c[...] + d[...])
    share = RHS // (XS * ZS)
    for z in range(ZS):
        cut[z, 2 * N : 3 * N] = total[N, :N]
        cut[z, 3 * N :] = jnp.zeros((24 - 3 * N, H), F32)
        for s in range(N):
            cut[z, share * s : share * (s + 1)] = total[s, share * z : share * (z + 1)]


def total_kernel(parts, mean_out, square_out):
    total = parts[0]
    for step in range(1, ZS):
        total = total + parts[step]
    for s in range(N):
        mean_out[s] = total[2 * s : 2 * s + 2]
    square_out[...] = total[2 * N : 3 * N]


def pair_kernel(mine, theirs, *outs):
    at = lax.axis_index("y")
    for step in range(YS):
        y = lax.rem(at + step, YS)
        outs[step][...] = mine[y] + theirs[y]


def q_sum_kernel(a, b, c, d, extra, out):
    for z in range(ZS):
        out[z, :NQ] = (a[z] + b[z]) + (c[z] + d[z])
        out[z, NQ] = jnp.concatenate([extra[z], jnp.zeros((FINE, WIDE - 128), F32)], axis=1)


def sum_kernel(a, b, c, d, *outs):
    at = lax.axis_index("x")
    for step in range(XS):
        x = lax.rem(at + step, XS)
        outs[step][...] = (a[x] + b[x]) + (c[x] + d[x])


def stack_kernel(*refs):
    out = refs[XS]
    at = lax.axis_index("x")
    for step in range(XS):
        out[lax.rem(at + XS - step, XS)] = refs[step][...]


def shifted(array, axis, step):
    size = lax.axis_size(axis)
    return lax.ppermute(array, axis, [(i, (i + step) % size) for i in range(size)])


def by_distance(array, axis):
    return [array] + [shifted(array, axis, step) for step in range(1, lax.axis_size(axis))]


def across(outs, axis):
    return [outs[0]] + [shifted(part, axis, step) for step, part in enumerate(outs) if step]


def row_gathered(array):
    near = by_distance(array, "y")
    return near + [shifted(piece, "core", 1) for piece in near]


def ringed(array, axis):
    size = lax.axis_size(axis)
    up, down = [array], [array]
    for _ in range(size // 2 - 1):
        up.append(shifted(up[-1], axis, 1))
        down.append(shifted(down[-1], axis, size - 1))
    half = array.shape[0] // 2
    return up + down[1:] + [shifted(up[-1][:half], axis, 1), shifted(down[-1][half:], axis, size - 1)]


def paired_rows(mine, other):
    outs = tuple(shape(*mine.shape[1:]) for _ in range(YS))
    theirs = shifted(other, "core", 1)
    parts = call(pair_kernel, outs, [VMEM] * 2, [], 6)(mine, theirs)
    return across(parts, "y")


def summed_rows(mine, other):
    outs = tuple(shape(*mine.shape[2:]) for _ in range(XS))
    parts = call(sum_kernel, outs, [VMEM] * YS, [], 6)(*paired_rows(mine, other))
    return across(parts, "x")


def stacked(pieces):
    return call(stack_kernel, shape(XS, *pieces[0].shape), [VMEM] * XS, [], 4)(*pieces)


def program(factor, diag, structure, parent, post):
    dma = pltpu.SemaphoreType.DMA
    blocks = jnp.transpose(factor, (0, 2, 3, 1))
    marks = jnp.transpose(structure, (0, 2, 1))
    thin = jnp.transpose(post, (0, 2, 1))
    fine = diag.reshape(N, RS, XS, ZS, FINE, H)
    q_pack, o_pack = call(
        pack_kernel,
        (shape(NQ * NARROW + 16, H), shape(NO, 2, NARROW, H)),
        [SMEM, SMEM, HBM, VMEM],
        [pltpu.VMEM((NQ + 2 * NO, NARROW, H), F32), dma((NQ + 2 * NO,))],
        60,
    )(parent, marks, blocks, thin)
    q_pieces = by_distance(q_pack, "x")
    o_pieces = ringed(o_pack, "z")

    def parts_of(*dims):
        return (shape(YS, *dims), shape(YS, *dims))

    q_mine, q_other, q_rhs = named(
        q_part_kernel,
        (*parts_of(ZS, NQ, FINE, WIDE), shape(ZS, FINE, 128)),
        [SMEM, VMEM, VMEM, VMEM, VMEM, HBM],
        [
            pltpu.VMEM((NQ, RS, ZS, FINE, H), F32),
            pltpu.VMEM((NQ, XS, NARROW, H), F32),
            pltpu.VMEM((YS, CS, ZS, FINE, WIDE), F32),
            pltpu.VMEM((128, H), F32),
            pltpu.VMEM((H, 128), F32),
            dma((NQ,)),
        ],
        50,
    )(parent, *q_pieces, fine)
    q_sum = call(q_sum_kernel, shape(ZS, NQ + 1, FINE, WIDE), [VMEM] * 5, [], 6)(*paired_rows(q_mine, q_other), q_rhs)
    q_all = row_gathered(lax.all_to_all(q_sum, "z", 0, 0, tiled=True))
    q_done = call(
        q_solve_kernel,
        shape(NQ, CHUNK, H),
        [SMEM] + [VMEM] * (2 * YS) + [HBM],
        [pltpu.VMEM((CHUNK, W), F32), pltpu.VMEM((NQ, RS, XS, ZS, FINE, H), F32), dma((NQ,))],
        50,
    )(parent, *q_all, fine)

    done_pieces = by_distance(q_done, "x")
    parts = pltpu.VMEM((YS, CS, XS, FINE, SLAB), F32)
    near_mine, near_other, base, o_wide = named(
        near_part_kernel,
        (*parts_of(XS, NO, FINE, SLAB), shape(NO, HALF, SLAB), shape(NO, SLAB, H)),
        [SMEM] + [VMEM] * 9 + [HBM],
        [
            pltpu.VMEM((NO, 2, ZS, NARROW, H), F32),
            parts,
            pltpu.VMEM((NO, 2, RS, XS, FINE, H), F32),
            dma((NO, 2)),
        ],
        44,
    )(parent, *o_pieces, fine)
    near_sum = summed_rows(near_mine, near_other)
    far_mine, far_other = call(
        far_part_kernel,
        parts_of(XS, NO, FINE, SLAB),
        [SMEM] + [VMEM] * 6,
        [pltpu.VMEM((NQ, RS, XS, FINE, H), F32), parts],
        14,
    )(parent, *done_pieces, base, o_wide)
    far_sum = summed_rows(far_mine, far_other)
    near_all = row_gathered(stacked(near_sum))
    far_near = by_distance(stacked(far_sum), "y")

    mean, square, load = call(
        near_solve_kernel,
        (shape(N, RHS, H), shape(N, 1, H), shape(N, RHS, CHUNK)),
        [SMEM] + [VMEM] * (4 * YS) + [VMEM, VMEM],
        [pltpu.VMEM((CHUNK, W), F32), pltpu.VMEM((CHUNK, 128), F32)],
        30,
    )(parent, *near_all, *q_all, fine, q_done)
    mean, square, load, *far_near = lax.optimization_barrier((mean, square, load, *far_near))
    far_all = far_near + [shifted(piece, "core", 1) for piece in far_near]
    packed = call(
        far_solve_kernel,
        tuple(shape(N + 1, RHS // XS, H) for _ in range(XS)),
        [SMEM] + [VMEM] * (2 * YS) + [VMEM] * 4,
        [pltpu.VMEM((N, RHS, H), F32), pltpu.VMEM((N, 1, H), F32), pltpu.VMEM((CHUNK, W), F32)],
        30,
    )(parent, *far_all, fine, mean, square, load)
    packed = call(
        turn_kernel, shape(ZS, 24, H), [VMEM] * XS, [pltpu.VMEM((N + 1, RHS // XS, H), F32)], 4
    )(*across(packed, "x"))
    mean_x, variance = call(total_kernel, (shape(N, 2, H), shape(N, H)), [VMEM], [], 4)(
        lax.all_to_all(packed, "z", 0, 0, tiled=True)
    )
    return jnp.transpose(mean_x, (0, 2, 1)), variance


def solution(mesh):
    finer = Mesh(mesh.devices.reshape(YS, CS, ZS, XS), (*ROW, *COL))
    placed = (
        P(None, ROW, None, COL),
        P(None, None, ROW),
        P(None, None, ROW),
        P(),
        P(None, ROW, COL),
    )
    return jax.shard_map(
        program,
        mesh=finer,
        in_specs=placed,
        out_specs=(P(None, ROW, COL), P(None, ROW)),
        check_vma=False,
    )
```

```python
import functools

import jax
import jax.numpy as jnp
from jax import lax
from jax.experimental import pallas as pl
from jax.experimental.pallas import tpu as pltpu
from jax.sharding import Mesh
from jax.sharding import PartitionSpec as P

ROW = ("y", "core")
COL = ("z", "x")
F32 = jnp.float32
BF16 = jnp.bfloat16

N = 6
W = 2048
H = 256
YS, CS, ZS, XS = 4, 2, 8, 4
RS = YS * CS
NARROW = W // (ZS * XS)
WIDE = NARROW * XS
STRIP = W // XS
CHUNK = STRIP // ZS
FINE = CHUNK // RS
RUN = STRIP // RS
HALF = W // ZS
SLAB = NARROW * ZS
NQ, NO = 2, 4
RHS = 64

SMEM = pl.BlockSpec(memory_space=pltpu.SMEM)
VMEM = pl.BlockSpec(memory_space=pltpu.VMEM)
HBM = pl.BlockSpec(memory_space=pltpu.HBM)


def call(kernel, outs, in_specs, scratch, mib, flops=10**9):
    return pl.pallas_call(
        kernel,
        out_shape=outs,
        cost_estimate=pl.CostEstimate(flops=flops, bytes_accessed=10**7, transcendentals=0),
        in_specs=in_specs,
        out_specs=jax.tree.map(lambda _: VMEM, outs),
        scratch_shapes=scratch,
        compiler_params=pltpu.CompilerParams(vmem_limit_bytes=mib * 1024 * 1024),
    )


def named(*args):
    def run(*operands):
        return call(*args)(*operands)

    return run


def shape(*dims):
    return jax.ShapeDtypeStruct(dims, F32)


def tree_of(parent_ref):
    par = [parent_ref[i] for i in range(N)]
    zero = jnp.int32(0)
    q, q_ok, o, o_ok = [zero] * NQ, [zero] * NQ, [zero] * NO, [zero] * NO
    q_count = o_count = zero
    for i in range(N):
        has_parent = (par[i] < N).astype(jnp.int32)
        has_child = zero
        for s in range(i):
            has_child = has_child | (par[s] == i).astype(jnp.int32)
        inner = has_parent * has_child
        outer = has_parent * (1 - has_child)
        for k in range(NQ):
            hit = inner * (q_count == k).astype(jnp.int32)
            q[k] = jnp.where(hit == 1, i, q[k])
            q_ok[k] = q_ok[k] | hit
        for k in range(NO):
            hit = outer * (o_count == k).astype(jnp.int32)
            o[k] = jnp.where(hit == 1, i, o[k])
            o_ok[k] = o_ok[k] | hit
        q_count = q_count + inner
        o_count = o_count + outer
    last = N - 1
    q_par = [jnp.minimum(parent_ref[v], last) for v in q]
    o_up = [parent_ref[v] for v in o]
    o_par = [jnp.minimum(v, last) for v in o_up]
    o_over = [jnp.where(up < N, parent_ref[v], N) for up, v in zip(o_up, o_par)]
    o_grand = [jnp.minimum(v, last) for v in o_over]
    o_deep = [ok * (v < N).astype(jnp.int32) for ok, v in zip(o_ok, o_over)]
    o_slot = [q_ok[1] * (v == q[1]).astype(jnp.int32) for v in o_par]
    return dict(
        q=q, q_ok=q_ok, q_par=q_par, o=o, o_ok=o_ok, o_par=o_par, o_grand=o_grand, o_deep=o_deep, o_slot=o_slot
    )


def at_index(values, index):
    result = values[0]
    for n in range(1, len(values)):
        result = jnp.where(index == n, values[n], result)
    return result


def each(number, step):
    def run(index, carry):
        step(index)
        return carry

    lax.fori_loop(0, number, run, 0)


def split(a):
    high = a.astype(BF16)
    return high, (a - high.astype(F32)).astype(BF16)


def dot3(a, b, transposed=False):
    dims = (((1,), (1 if transposed else 0,)), ((), ()))
    mul = lambda u, v: lax.dot_general(u, v, dims, preferred_element_type=F32)
    ah, al = a
    bh, bl = b
    return mul(ah, bh) + (mul(ah, bl) + mul(al, bh))


def masked_rows(block, row_of):
    rows = row_of(lax.broadcasted_iota(jnp.int32, block.shape, 0))
    cols = lax.axis_index(ROW) * H + lax.broadcasted_iota(jnp.int32, block.shape, 1)
    return jnp.where(rows >= cols, block, 0.0)


def put_row_parts(part, index, mine, other, parts):
    core = lax.axis_index("core")
    parts[...] = part.reshape(parts.shape)
    mine[:, :, index] = parts[:, core]
    other[:, :, index] = parts[:, 1 - core]


def pack_kernel(parent, marks, factor, thin, q_out, o_out, held, sems):
    t = tree_of(parent)
    slots = [(t["q_par"][k], t["q"][k], t["q_ok"][k]) for k in range(NQ)]
    for j in range(NO):
        slots.append((t["o_par"][j], t["o"][j], t["o_ok"][j]))
        slots.append((t["o_grand"][j], t["o"][j], t["o_deep"][j]))
    copies = []
    for n, (up, node, _) in enumerate(slots):
        copies.append(pltpu.make_async_copy(factor.at[up, node], held.at[n], sems.at[n]))
        copies[-1].start()
    left = lax.broadcasted_iota(jnp.int32, (NARROW, H), 1) < H // 2
    for s in range(N):
        q_out[NQ * NARROW + 2 * s : NQ * NARROW + 2 * s + 2] = thin[s]
    q_out[NQ * NARROW + 2 * N :] = jnp.zeros((16 - 2 * N, H), F32)
    for n, (up, node, ok) in enumerate(slots):
        copies[n].wait()
        first = (marks[node, 0, up] * ok).astype(F32)
        second = (marks[node, 1, up] * ok).astype(F32)
        block = held[n] * jnp.where(left, first, second)
        if n < NQ:
            q_out[n * NARROW : (n + 1) * NARROW] = block
        else:
            o_out[(n - NQ) // 2, (n - NQ) % 2] = block


def q_part_kernel(parent, p0, p1, p2, p3, diag, mine, other, rhs_out, strip, wide, parts, thin, tall, sems):
    t = tree_of(parent)
    at = lax.axis_index("x")
    copies = []
    for k in range(NQ):
        copies.append(pltpu.make_async_copy(diag.at[t["q_par"][k], :, at], strip.at[k], sems.at[k]))
        copies[-1].start()
    row_of = lambda i: (i // RUN) * H + at * RUN + i % RUN
    thin[...] = jnp.zeros_like(thin)
    for step, piece in enumerate((p0, p1, p2, p3)):
        source = lax.rem(at + XS - step, XS)
        for k in range(NQ):
            wide[k, source] = piece[k * NARROW : (k + 1) * NARROW]
        thin[pl.ds(pl.multiple_of(source * 16, 16), 16)] = piece[NQ * NARROW :]
    tall[...] = thin[...].T
    rhs_out[...] = tall[pl.ds(pl.multiple_of(at * RUN, RUN), RUN)].reshape(ZS, FINE, 128)
    for k in range(NQ):
        copies[k].wait()

    @functools.partial(each, NQ)
    def _(k):
        left = split(masked_rows(strip[k].reshape(STRIP, H), row_of))
        part = -dot3(left, split(wide[k].reshape(WIDE, H)), True)
        put_row_parts(part, k, mine, other, parts)


def sides(pieces, step, core_at):
    return ((core_at, pieces[0].at[step]), (1 - core_at, pieces[1].at[step]))


def q_solve_kernel(parent, *refs):
    pieces, (diag, out, rows, held, sems) = refs[:2], refs[2:]
    t = tree_of(parent)
    copies = []
    for k in range(NQ):
        copies.append(pltpu.make_async_copy(diag.at[t["q"][k]], held.at[k], sems.at[k]))
        copies[-1].start()
    for k in range(NQ):
        copies[k].wait()

    @functools.partial(each, NQ)
    def _(k):
        y_at, core_at = lax.axis_index("y"), lax.axis_index("core")
        for step in range(YS):
            y = lax.rem(y_at + YS - step, YS)
            for side, source in sides(pieces, step, core_at):
                first = pl.multiple_of((y * CS + side) * FINE, FINE)
                for z in range(ZS):
                    rows[z // 2, pl.ds(first, FINE), z % 2 * WIDE : (z % 2 + 1) * WIDE] = source[z, k]

        def add(n, done):
            block = masked_rows(held[k, pl.ds(2 * n, 2)].reshape(2 * WIDE, H), lambda i: 2 * WIDE * n + i)
            return done + dot3(split(rows[n]), split(block))

        out[k] = lax.fori_loop(0, ZS // 2, add, jnp.zeros((CHUNK, H), F32), unroll=2)


def outer_solve(pieces, j, node, diag, rows, unroll):
    y_at, core_at = lax.axis_index("y"), lax.axis_index("core")
    for step in range(YS):
        y = lax.rem(y_at + YS - step, YS)
        for side, source in sides(pieces, step, core_at):
            first = pl.multiple_of((y * CS + side) * FINE, FINE)
            rows[:, pl.ds(first, FINE)] = source[:, j]

    def add(x, done):
        block = masked_rows(
            diag[node, :, x].reshape(SLAB, H), lambda i: (i // NARROW) * WIDE + x * NARROW + i % NARROW
        )
        return done + dot3(split(rows[x]), split(block))

    return lax.fori_loop(0, XS, add, jnp.zeros((CHUNK, H), F32), unroll=unroll)


def near_part_kernel(parent, *refs):
    own, u1, u2, u3, d1, d2, d3, u4 = refs[:8]
    diag, mine, other, base_out, wide_out, wide, parts, strip, sems = refs[8:]
    t = tree_of(parent)
    at = lax.axis_index("z")
    copies = []
    for j in range(NO):
        for e, node in enumerate((t["o_par"][j], t["o_grand"][j])):
            copies.append(pltpu.make_async_copy(diag.at[node, :, :, at], strip.at[j, e], sems.at[j, e]))
            copies[-1].start()
    for step, piece in ((0, own), (1, u1), (2, u2), (3, u3), (-1, d1), (-2, d2), (-3, d3), (4, u4)):
        source = lax.rem(at + ZS - step, ZS)
        for j in range(NO):
            for e in range(2):
                wide[j, e, source] = piece[j, e]
    row_of = lambda i: (i // (XS * FINE)) * H + (i // FINE) % XS * RUN + at * FINE + i % FINE
    for j in range(NO):
        for e in range(2):
            copies[2 * j + e].wait()

    @functools.partial(each, NO)
    def _(j):
        for e in range(2):
            left = split(masked_rows(strip[j, e].reshape(HALF, H), row_of))
            right = wide[j, e].reshape(SLAB, H)
            part = -dot3(left, split(right), True)
            if e == 0:
                put_row_parts(part, j, mine, other, parts)
                wide_out[j] = right * at_index(t["o_deep"], j).astype(F32)
            else:
                base_out[j] = part


def far_part_kernel(parent, a, b, c, d, base, wide, mine, other, tall, parts):
    t = tree_of(parent)
    at = lax.axis_index("x")
    for step, piece in enumerate((a, b, c, d)):
        source = lax.rem(at + XS - step, XS)
        for k in range(NQ):
            tall[k, :, source] = piece[k].reshape(RS, FINE, H)

    @functools.partial(each, NO)
    def _(j):
        left = split(tall[at_index(t["o_slot"], j)].reshape(HALF, H))
        part = base[j] - dot3(left, split(wide[j]), True)
        put_row_parts(part, j, mine, other, parts)


def near_solve_kernel(parent, *refs):
    pieces, q_pieces = refs[:2], refs[2:4]
    diag, q_done, mean_out, square_out, load, rows, thin = refs[4:]
    t = tree_of(parent)
    x_at, z_at = lax.axis_index("x"), lax.axis_index("z")
    y_at, core_at = lax.axis_index("y"), lax.axis_index("core")
    for z in range(ZS):
        for step in range(YS):
            y = lax.rem(y_at + YS - step, YS)
            for side, source in sides(q_pieces, step, core_at):
                at = pl.multiple_of((y * CS + side) * FINE, FINE)
                thin[pl.ds(at, FINE)] = source[z, NQ][:, :128]
        flat = thin[...].T
        for x in range(XS):
            for s in range(N):
                to = 16 * x + 2 * z
                load[s, to : to + 2] = flat[16 * x + 2 * s : 16 * x + 2 * s + 2]
    for s in range(N):
        block = masked_rows(
            diag[s, :, x_at, z_at].reshape(CHUNK, H), lambda i: (i // FINE) * H + x_at * RUN + z_at * FINE + i % FINE
        )
        mean_out[s] = dot3(split(load[s]), split(block))
        square_out[s] = jnp.sum(block * block, axis=0, keepdims=True)
    for k in range(NQ):
        node = t["q"][k]
        done = q_done[k]
        mean_out[node] += dot3(split(load[t["q_par"][k]]), split(done))
        square_out[node] += jnp.sum(done * done, axis=0, keepdims=True)

    @functools.partial(each, NO)
    def _(j):
        node = at_index(t["o"], j)
        done = outer_solve(pieces, j, node, diag, rows, 1)
        mean_out[node] += dot3(split(load[at_index(t["o_par"], j)]), split(done))
        square_out[node] += jnp.sum(done * done, axis=0, keepdims=True)


def far_solve_kernel(parent, *refs):
    pieces = refs[:2]
    diag, mean_in, square_in, load, out, mean, square, rows = refs[2:]
    t = tree_of(parent)
    mean[...] = mean_in[...]
    square[...] = square_in[...]

    @functools.partial(each, NO)
    def _(j):
        node = at_index(t["o"], j)
        done = outer_solve(pieces, j, node, diag, rows, 2)
        mean[node] += dot3(split(load[at_index(t["o_grand"], j)]), split(done))
        square[node] += jnp.sum(done * done, axis=0, keepdims=True)

    share = RHS // XS
    for x in range(XS):
        for s in range(N):
            out[x, s] = mean[s, x * share : (x + 1) * share]
            out[x, N, s : s + 1] = square[s]
        out[x, N, N:] = jnp.zeros((share - N, H), F32)


def turn_kernel(parts, cut, total):
    total[...] = (parts[0] + parts[1]) + (parts[2] + parts[3])
    share = RHS // (XS * ZS)
    for z in range(ZS):
        cut[z, 2 * N : 3 * N] = total[N, :N]
        cut[z, 3 * N :] = jnp.zeros((24 - 3 * N, H), F32)
        for s in range(N):
            cut[z, share * s : share * (s + 1)] = total[s, share * z : share * (z + 1)]


def total_kernel(parts, mean_out, square_out):
    total = parts[0]
    for step in range(1, ZS):
        total = total + parts[step]
    for s in range(N):
        mean_out[s] = total[2 * s : 2 * s + 2]
    square_out[...] = total[2 * N : 3 * N]


def pair_kernel(mine, theirs, *outs):
    at = lax.axis_index("y")
    for step in range(YS):
        y = lax.rem(at + step, YS)
        outs[step][...] = mine[y] + theirs[y]


def q_sum_kernel(a, b, c, d, extra, out):
    for z in range(ZS):
        out[z, :NQ] = (a[z] + b[z]) + (c[z] + d[z])
        out[z, NQ] = jnp.concatenate([extra[z], jnp.zeros((FINE, WIDE - 128), F32)], axis=1)


def sum_kernel(a, b, c, d, *outs):
    at = lax.axis_index("x")
    for step in range(XS):
        x = lax.rem(at + step, XS)
        outs[step][...] = (a[x] + b[x]) + (c[x] + d[x])


def stack_kernel(*refs):
    out = refs[XS]
    at = lax.axis_index("x")
    for step in range(XS):
        out[lax.rem(at + XS - step, XS)] = refs[step][...]


def shifted(array, axis, step):
    size = lax.axis_size(axis)
    return lax.ppermute(array, axis, [(i, (i + step) % size) for i in range(size)])


def by_distance(array, axis):
    return [array] + [shifted(array, axis, step) for step in range(1, lax.axis_size(axis))]


def across(outs, axis):
    return [outs[0]] + [shifted(part, axis, step) for step, part in enumerate(outs) if step]


def ringed(array, axis):
    size = lax.axis_size(axis)
    up, down = [array], [array]
    for _ in range(size // 2 - 1):
        up.append(shifted(up[-1], axis, 1))
        down.append(shifted(down[-1], axis, size - 1))
    return up + down[1:] + [shifted(up[-1], axis, 1)]


def paired_rows(mine, other):
    outs = tuple(shape(*mine.shape[1:]) for _ in range(YS))
    theirs = shifted(other, "core", 1)
    parts = call(pair_kernel, outs, [VMEM] * 2, [], 6)(mine, theirs)
    return across(parts, "y")


def summed_rows(mine, other):
    outs = tuple(shape(*mine.shape[2:]) for _ in range(XS))
    parts = call(sum_kernel, outs, [VMEM] * YS, [], 6)(*paired_rows(mine, other))
    return across(parts, "x")


def stacked(pieces):
    return call(stack_kernel, shape(XS, *pieces[0].shape), [VMEM] * XS, [], 4)(*pieces)


def program(factor, diag, structure, parent, post):
    dma = pltpu.SemaphoreType.DMA
    blocks = jnp.transpose(factor, (0, 2, 3, 1))
    marks = jnp.transpose(structure, (0, 2, 1))
    thin = jnp.transpose(post, (0, 2, 1))
    fine = diag.reshape(N, RS, XS, ZS, FINE, H)
    q_pack, o_pack = call(
        pack_kernel,
        (shape(NQ * NARROW + 16, H), shape(NO, 2, NARROW, H)),
        [SMEM, SMEM, HBM, VMEM],
        [pltpu.VMEM((NQ + 2 * NO, NARROW, H), F32), dma((NQ + 2 * NO,))],
        62,
    )(parent, marks, blocks, thin)
    q_pieces = by_distance(q_pack, "x")
    o_pieces = ringed(o_pack, "z")

    def parts_of(*dims):
        return (shape(YS, *dims), shape(YS, *dims))

    q_mine, q_other, q_rhs = named(
        q_part_kernel,
        (*parts_of(ZS, NQ, FINE, WIDE), shape(ZS, FINE, 128)),
        [SMEM, VMEM, VMEM, VMEM, VMEM, HBM],
        [
            pltpu.VMEM((NQ, RS, ZS, FINE, H), F32),
            pltpu.VMEM((NQ, XS, NARROW, H), F32),
            pltpu.VMEM((YS, CS, ZS, FINE, WIDE), F32),
            pltpu.VMEM((128, H), F32),
            pltpu.VMEM((H, 128), F32),
            dma((NQ,)),
        ],
        50,
    )(parent, *q_pieces, fine)
    q_sum = call(q_sum_kernel, shape(ZS, NQ + 1, FINE, WIDE), [VMEM] * 5, [], 6)(*paired_rows(q_mine, q_other), q_rhs)
    q_near = jnp.stack(by_distance(lax.all_to_all(q_sum, "z", 0, 0, tiled=True), "y"))
    q_all = [q_near, shifted(q_near, "core", 1)]
    q_done = call(
        q_solve_kernel,
        shape(NQ, CHUNK, H),
        [SMEM] + [VMEM] * 2 + [HBM],
        [
            pltpu.VMEM((ZS // 2, CHUNK, 2 * WIDE), F32),
            pltpu.VMEM((NQ, RS, XS, ZS, FINE, H), F32),
            dma((NQ,)),
        ],
        50,
    )(parent, *q_all, fine)

    done_pieces = by_distance(q_done, "x")
    parts = pltpu.VMEM((YS, CS, XS, FINE, SLAB), F32)
    near_mine, near_other, base, o_wide = named(
        near_part_kernel,
        (*parts_of(XS, NO, FINE, SLAB), shape(NO, HALF, SLAB), shape(NO, SLAB, H)),
        [SMEM] + [VMEM] * 8 + [HBM],
        [
            pltpu.VMEM((NO, 2, ZS, NARROW, H), F32),
            parts,
            pltpu.VMEM((NO, 2, RS, XS, FINE, H), F32),
            dma((NO, 2)),
        ],
        40,
    )(parent, *o_pieces, fine)
    near_sum = summed_rows(near_mine, near_other)
    far_mine, far_other = call(
        far_part_kernel,
        parts_of(XS, NO, FINE, SLAB),
        [SMEM] + [VMEM] * 6,
        [pltpu.VMEM((NQ, RS, XS, FINE, H), F32), parts],
        14,
    )(parent, *done_pieces, base, o_wide)
    far_sum = summed_rows(far_mine, far_other)
    near_pieces = by_distance(stacked(near_sum), "y")
    far_turned = stacked(far_sum)
    far_pieces = by_distance(far_turned, "y")
    *near_pieces, _ = lax.optimization_barrier((*near_pieces, far_turned))
    near_stack = jnp.stack(near_pieces)
    near_all = [near_stack, shifted(near_stack, "core", 1)]

    mean, square, load = call(
        near_solve_kernel,
        (shape(N, RHS, H), shape(N, 1, H), shape(N, RHS, CHUNK)),
        [SMEM] + [VMEM] * 4 + [VMEM, VMEM],
        [pltpu.VMEM((XS, CHUNK, SLAB), F32), pltpu.VMEM((CHUNK, 128), F32)],
        30,
    )(parent, *near_all, *q_all, fine, q_done)
    mean, square, load, *far_pieces = lax.optimization_barrier((mean, square, load, *far_pieces))
    far_near = jnp.stack(far_pieces)
    far_all = [far_near, shifted(far_near, "core", 1)]
    packed = call(
        far_solve_kernel,
        shape(XS, N + 1, RHS // XS, H),
        [SMEM] + [VMEM] * 6,
        [pltpu.VMEM((N, RHS, H), F32), pltpu.VMEM((N, 1, H), F32), pltpu.VMEM((XS, CHUNK, SLAB), F32)],
        30,
    )(parent, *far_all, fine, mean, square, load)
    packed = call(
        turn_kernel, shape(ZS, 24, H), [VMEM], [pltpu.VMEM((N + 1, RHS // XS, H), F32)], 4
    )(lax.all_to_all(packed, "x", 0, 0, tiled=True))
    mean_x, variance = call(total_kernel, (shape(N, 2, H), shape(N, H)), [VMEM], [], 4)(
        lax.all_to_all(packed, "z", 0, 0, tiled=True)
    )
    return jnp.transpose(mean_x, (0, 2, 1)), variance


def solution(mesh):
    finer = Mesh(mesh.devices.reshape(YS, CS, ZS, XS), (*ROW, *COL))
    placed = (
        P(None, ROW, None, COL),
        P(None, None, ROW),
        P(None, None, ROW),
        P(),
        P(None, ROW, COL),
    )
    return jax.shard_map(
        program,
        mesh=finer,
        in_specs=placed,
        out_specs=(P(None, ROW, COL), P(None, ROW)),
        check_vma=False,
    )
```
